256 devices in a mesh: dp: 4 (over y), ep: 64 (over z, x, core).
Axes of the slice: x: 4, y: 4, z: 8, core: 2. Of those that a mesh axis runs over, the one named last changes fastest.
Arguments:
- tokens: bfloat16 [32768, 7168], P(('dp', 'ep')), may hold values from -6 to 6
- out_grad: bfloat16 [32768, 7168], P(('dp', 'ep')), may hold values from -3 to 3
- route_weight: float32 [32768, 1], P(('dp', 'ep')), may hold values from 0.2 to 1
- expert_ids: int32 [32768, 1], P(('dp', 'ep')), may hold values from 0 to 15
- w_gate: bfloat16 [1024, 114688], P('dp', 'ep'), may hold values from -0.0625 to 0.0625
- w_up: bfloat16 [1024, 114688], P('dp', 'ep'), may hold values from -0.0625 to 0.0625
- w_down: bfloat16 [1024, 114688], P('dp', 'ep'), may hold values from -0.1875 to 0.1875
Outputs:
- in_grad: bfloat16 [32768, 7168], P(('dp', 'ep'))
- grad_gate: bfloat16 [1024, 114688], P('dp', 'ep')
- grad_up: bfloat16 [1024, 114688], P('dp', 'ep')
- grad_down: bfloat16 [1024, 114688], P('dp', 'ep')
The draws below stay inside these ranges and needn't reach their ends.
All inputs are finite; a program needn't handle non-finite values.
Results may differ from the reference program's by a relative error of at most 0.012.
Values may be sent and summed in bfloat16 or wider, within the bound.
A program may use at most 128 MiB of HBM per device.

```python
import jax
import jax.numpy as jnp
from jax import lax

D = 7168
FF = 1024
GROUP = 4
TOP = 1
TOK_DEV = 128
EXPERTS = 16
CAP = 6
TOKENS = 32768
N_DP = 4
N_EP = 64


def shard_levels(key, dims, pieces, low, top_value):
    factor_of, own = 1.0, jax.random.fold_in(key, 6)
    for dim, parts in pieces:
        heights = jnp.exp(jax.random.uniform(jax.random.fold_in(own, dim), (parts,), jnp.float32, low / len(pieces), top_value / len(pieces)))
        factor_of = factor_of * jnp.repeat(heights, dims[dim] // parts).reshape([-1 if axis == dim else 1 for axis in range(len(dims))])
    return factor_of


def picks_of(own_key, rows, count, top, lift):
    sequence = jax.random.permutation(jax.random.fold_in(own_key, 1), count)
    pull = sequence
    for power in range(3):
        pull = pull * pull // count
    pull = pull * lift // count
    chance = jax.random.randint(jax.random.fold_in(own_key, 2), (rows, count), 0, 4096) + pull
    fixed_rows = jax.random.permutation(jax.random.fold_in(own_key, 3), rows)[jnp.arange(count) % rows]
    chance = jnp.where(jnp.arange(rows)[:, None] == fixed_rows[None, :], 1 << 14, chance)
    score = chance * count + jnp.arange(count)
    return lax.top_k(score.astype(jnp.int32), top)[1].astype(jnp.int32)


def centred(rng, dims, width, most, cuts=(), held_as=jnp.bfloat16):
    drawn = width * jax.random.normal(rng, dims, jnp.float32)
    if cuts:
        drawn = drawn * shard_levels(rng, dims, cuts, -0.22, 0.18)
    return jnp.clip(drawn, -most, most).astype(held_as)


def setup_inputs(seed: int = 0) -> dict:
    splits = jax.random.split(jax.random.key(seed), 8)
    tokens = centred(splits[0], (TOKENS, D), 1.0, 6.0, ((0, 256),))
    out_grad = centred(splits[1], (TOKENS, D), 0.5, 3.0, ((0, 256),))
    route_weight = jnp.clip(0.2 + 0.8 * jax.random.uniform(splits[2], (TOKENS, TOP), jnp.float32) ** shard_levels(splits[2], (TOKENS, TOP), ((0, 256),), -0.2, 0.2), 0.2, 1.0)
    expert_ids = picks_of(splits[3], TOKENS, EXPERTS, TOP, 1024)
    w_gate = centred(splits[4], (FF, EXPERTS * D), D ** -0.5, 0.0625, ((0, 4), (1, 64)))
    w_up = centred(splits[5], (FF, EXPERTS * D), D ** -0.5, 0.0625, ((0, 4), (1, 64)))
    w_down = centred(splits[6], (FF, EXPERTS * D), FF ** -0.5, 0.1875, ((0, 4), (1, 64)))
    return {"tokens": tokens, "out_grad": out_grad, "route_weight": route_weight, "expert_ids": expert_ids, "w_gate": w_gate, "w_up": w_up, "w_down": w_down}


CONTRACT_LAST = (((1,), (1,)), ((), ()))
CONTRACT_FIRST = (((0,), (0,)), ((), ()))


def slot_tables(expert_ids, route_weight, experts, capacity):
    token_count, top_count = expert_ids.shape
    pair_count = token_count * top_count
    flat_ids = expert_ids.reshape(pair_count)
    onehot = (flat_ids[:, None] == jnp.arange(experts, dtype=jnp.int32)[None, :]).astype(jnp.int32)
    before = jnp.cumsum(onehot, axis=0) - onehot
    ranks = jnp.sum(before * onehot, axis=1)
    kept = ranks < capacity
    slots = jnp.where(kept, flat_ids * capacity + ranks, 0).astype(jnp.int32)
    slot_ids = jnp.arange(experts * capacity, dtype=jnp.int32)
    match = (slots[None, :] == slot_ids[:, None]) & kept[None, :]
    pair_ids = jnp.arange(pair_count, dtype=jnp.int32)
    pair_of_slot = jnp.sum(jnp.where(match, pair_ids[None, :], 0), axis=1).astype(jnp.int32)
    filled = jnp.any(match, axis=1)
    flat_weight = route_weight.reshape(pair_count)
    weight_of_slot = jnp.sum(jnp.where(match, flat_weight[None, :], jnp.float32(0.0)), axis=1)
    return kept, slots, pair_of_slot // top_count, filled, weight_of_slot


def source_slots(tokens, out_grad, route_weight, expert_ids):
    kept, slots, token_of_slot, filled, weight_of_slot = slot_tables(expert_ids, route_weight, EXPERTS, CAP)
    x_slots = jnp.take(tokens, token_of_slot, axis=0) * filled[:, None].astype(jnp.bfloat16)
    d_slots = (jnp.take(out_grad, token_of_slot, axis=0).astype(jnp.float32) * weight_of_slot[:, None]).astype(jnp.bfloat16)
    return x_slots, d_slots, kept, slots


def quarter_sum(left, weight):
    quarter = D // GROUP
    total = jnp.zeros((left.shape[0], weight.shape[0]), jnp.float32)
    for piece in range(GROUP):
        part = lax.dot_general(left[:, piece * quarter:(piece + 1) * quarter], weight[:, piece * quarter:(piece + 1) * quarter], CONTRACT_LAST, preferred_element_type=jnp.float32)
        total = total + lax.optimization_barrier(part.astype(jnp.bfloat16)).astype(jnp.float32)
    return total


def activations(gate, up, back):
    logistic = jax.nn.sigmoid(gate)
    silu = gate * logistic
    hidden = (silu * up).astype(jnp.bfloat16)
    d_gate = (back * up * logistic * (1.0 + gate * (1.0 - logistic))).astype(jnp.bfloat16)
    d_up = (back * silu).astype(jnp.bfloat16)
    return hidden, d_gate, d_up


def expert_work(operands):
    x_rows, d_rows, gate_w, up_w, down_w = operands
    gate = quarter_sum(x_rows, gate_w)
    up = quarter_sum(x_rows, up_w)
    back = quarter_sum(d_rows, down_w)
    hidden, d_gate, d_up = activations(gate, up, back)
    expert_dx = (jnp.dot(d_gate, gate_w, preferred_element_type=jnp.float32) + jnp.dot(d_up, up_w, preferred_element_type=jnp.float32)).astype(jnp.bfloat16)
    gate_term = lax.dot_general(d_gate, x_rows, CONTRACT_FIRST, preferred_element_type=jnp.float32).astype(jnp.bfloat16)
    up_term = lax.dot_general(d_up, x_rows, CONTRACT_FIRST, preferred_element_type=jnp.float32).astype(jnp.bfloat16)
    down_term = lax.dot_general(hidden, d_rows, CONTRACT_FIRST, preferred_element_type=jnp.float32).astype(jnp.bfloat16)
    return expert_dx, gate_term, up_term, down_term


def reference(tokens, out_grad, route_weight, expert_ids, w_gate, w_up, w_down):
    sources = N_DP * N_EP
    x_src = tokens.reshape(sources, TOK_DEV, D)
    d_src = out_grad.reshape(sources, TOK_DEV, D)
    w_src = route_weight.reshape(sources, TOK_DEV, TOP)
    i_src = expert_ids.reshape(sources, TOK_DEV, TOP)
    x_slots, d_slots, kept, slots = jax.vmap(source_slots)(x_src, d_src, w_src, i_src)
    x_slots = x_slots.reshape(N_DP, N_EP, EXPERTS, CAP, D)
    d_slots = d_slots.reshape(N_DP, N_EP, EXPERTS, CAP, D)
    gate_e = w_gate.reshape(FF, EXPERTS, D).transpose(1, 0, 2)
    up_e = w_up.reshape(FF, EXPERTS, D).transpose(1, 0, 2)
    down_e = w_down.reshape(FF, EXPERTS, D).transpose(1, 0, 2)
    grad_sums = [jnp.zeros((EXPERTS, FF, D), jnp.float32) for which in range(3)]
    returned = []
    for row in range(N_DP):
        x_rows = x_slots[row].transpose(1, 0, 2, 3).reshape(EXPERTS, N_EP * CAP, D)
        d_rows = d_slots[row].transpose(1, 0, 2, 3).reshape(EXPERTS, N_EP * CAP, D)
        expert_dx, gate_term, up_term, down_term = lax.map(expert_work, (x_rows, d_rows, gate_e, up_e, down_e))
        grad_sums = [grad_sums[0] + gate_term.astype(jnp.float32), grad_sums[1] + up_term.astype(jnp.float32), grad_sums[2] + down_term.astype(jnp.float32)]
        returned.append(expert_dx.reshape(EXPERTS, N_EP, CAP, D).transpose(1, 0, 2, 3).reshape(N_EP, EXPERTS * CAP, D))
    slot_rows = jnp.stack(returned, axis=0).reshape(sources, EXPERTS * CAP, D)

    def gather_back(rows, kept_one, slots_one):
        pair_rows = jnp.take(rows, slots_one, axis=0) * kept_one[:, None].astype(jnp.bfloat16)
        return jnp.sum(pair_rows.reshape(TOK_DEV, TOP, D).astype(jnp.float32), axis=1).astype(jnp.bfloat16)

    in_grad = jax.vmap(gather_back)(slot_rows, kept, slots).reshape(TOK_DEV * sources, D)
    outs = [total.astype(jnp.bfloat16).transpose(1, 0, 2).reshape(FF, EXPERTS * D) for total in grad_sums]
    return in_grad, outs[0], outs[1], outs[2]
```

```python
import functools

import jax
import jax.numpy as jnp
from jax import lax
from jax.experimental import pallas as pl
from jax.experimental.pallas import tpu as pltpu
from jax.sharding import PartitionSpec as P

D = 7168
GROUP = 4
CAP = 6
PLANE = 8
NT = (((1,), (1,)), ((), ()))
NN = (((1,), (0,)), ((), ()))
MESH = pl.DeviceIdType.MESH
BF = jnp.bfloat16
F32 = jnp.float32


class Copies:
    def __init__(self, send, recv):
        self.send, self.recv, self.used, self.open = send, recv, 0, []

    def slots(self, count):
        first = self.used
        self.used += count
        return first

    def make(self, src, dst, slot, device):
        return pltpu.make_async_remote_copy(
            src_ref=src,
            dst_ref=dst,
            send_sem=self.send.at[slot],
            recv_sem=self.recv.at[slot],
            device_id=device,
            device_id_type=MESH,
        )

    def start(self, src, dst, slot, device):
        copy = self.make(src, dst, slot, device)
        copy.start()
        self.open.append(copy)

    def arrived(self, dst, slot, device):
        self.make(dst, dst, slot, device).wait_recv()

    def drain(self):
        for copy in self.open:
            copy.wait_send()


def halves(width):
    return [(0, width // 2), (width // 2, width // 2)]


def pieces(width):
    unit = width // 7
    return [(0, 2 * unit), (2 * unit, 2 * unit), (4 * unit, 2 * unit), (6 * unit, unit)]


def semaphores(planes, plane):
    count = 4 * (plane - 1) + 4 * (planes - 1) + 4 * planes + 3 + 4 + 4 + 12 + 3
    return count + 4 + 4 * (planes - 1) + 4 * (plane - 1)


def kernel(
    planes, plane, cap,
    sel_ref, sel_t_ref, scale_ref, perm_ref, perm_t_ref,
    tok_hbm, grad_hbm, wg_hbm, wu_hbm, wd_hbm,
    out_ref, gout_ref,
    raw, send1, r1, r1p, xs, wv, gu_send, gu_recv, gu_keep, gu_send2, gu_recv2,
    bk_send, bk_recv, bk_keep, bk_send2, bk_recv2, gu_own, hid, dgu, dt,
    gterm, grecv, dx_send, dx_recv, dx_own, dxs, rz, rzp, ret,
    local_sem, send_sem, recv_sem,
):
    quarter = xs.shape[2]
    block = planes * cap
    rows = plane * block
    part = rows // 4
    units = wv.shape[1] // 2
    r = lax.axis_index("dp")
    ep = lax.axis_index("ep")
    z = ep // plane
    u = lax.rem(ep, plane)
    c = lax.rem(u, 2)
    bx = lax.rem(u // 2, 2)
    y_tok = r + 1 - 2 * lax.rem(r, 2)
    y_wt = 3 - r
    copies = Copies(send_sem, recv_sem)

    def in_plane(k):
        if k == 0:
            return u
        out = u
        for bit in range(3):
            if k >> bit & 1:
                out = out + (1 << bit) * (1 - 2 * lax.rem(u // (1 << bit), 2))
        return out

    def at_u(k):
        return (r, z * plane + in_plane(k))

    def z_to(k):
        return lax.rem(z + k, planes)

    def z_from(k):
        return lax.rem(z + planes - k, planes)

    def at_z(k):
        return (r, z_to(k) * plane + u)

    def from_z(k):
        return (r, z_from(k) * plane + u)

    def blk(index, size=None):
        size = block if size is None else size
        return pl.ds(pl.multiple_of(index * size, size), size)

    z_order = [1, planes - 1]
    for k in range(2, planes):
        if k not in z_order:
            z_order.append(k)
            if planes - k not in z_order:
                z_order.append(planes - k)
    z_order = list(dict.fromkeys(k for k in z_order if k % planes))
    u_order = [k for k in (4, 5, 2, 3, 6, 7, 1) if k < plane]
    token_y, weight_y = (y_tok, ep), (y_wt, ep)

    loads = [
        pltpu.make_async_copy(tok_hbm, raw.at[0], local_sem.at[0]),
        pltpu.make_async_copy(grad_hbm, raw.at[1], local_sem.at[1]),
    ]
    for w, ref in enumerate((wg_hbm, wu_hbm, wd_hbm)):
        loads.append(pltpu.make_async_copy(ref, wv.at[w, pl.ds(0, units)], local_sem.at[2 + w]))
    for load in loads:
        load.start()

    barrier = pltpu.get_barrier_semaphore()
    partners = [at_u(k) for k in u_order] + [at_z(k) for k in z_order] + [token_y, weight_y]
    for device in partners:
        pl.semaphore_signal(barrier, inc=1, device_id=device, device_id_type=MESH)
    pl.semaphore_wait(barrier, len(partners))

    w_slot = copies.slots(3)
    for w, ref in enumerate((wg_hbm, wu_hbm, wd_hbm)):
        copies.start(ref, wv.at[w, pl.ds(units, units)], w_slot + w, weight_y)

    chunks = halves(quarter)
    st1 = copies.slots(4 * (plane - 1))
    st2 = copies.slots(4 * (planes - 1))
    fwd = copies.slots(4 * planes)

    def gather(a, j):
        lo, width = chunks[j]
        for q in range(GROUP):
            got = lax.dot_general(
                sel_ref[...], raw[a, :, pl.ds(q * quarter + lo, width)], NN, preferred_element_type=F32
            )
            if a:
                got = got * scale_ref[...]
            got = got.astype(BF)
            for h in range(plane // GROUP):
                send1[a, h * GROUP + q, :, pl.ds(lo, width)] = got[h * block : (h + 1) * block]
        cols = pl.ds(lo, width)
        for k in u_order:
            copies.start(
                send1.at[a, in_plane(k), :, cols],
                r1.at[a, blk(u), cols],
                st1 + (2 * a + j) * (plane - 1) + k - 1,
                at_u(k),
            )
        r1[a, blk(u), cols] = send1[a, u, :, cols]

    def plane_stage(a, j):
        lo, width = chunks[j]
        cols = pl.ds(lo, width)
        for k in u_order:
            copies.arrived(
                r1.at[a, blk(in_plane(k)), cols], st1 + (2 * a + j) * (plane - 1) + k - 1, at_u(k)
            )
        r1p[a, :, cols] = lax.dot_general(
            perm_ref[...], r1[a, :, cols], NN, preferred_element_type=F32
        ).astype(BF)
        for k in z_order:
            copies.start(
                r1p.at[a, blk(z_to(k)), cols],
                xs.at[a, blk(z), cols],
                st2 + (2 * a + j) * (planes - 1) + k - 1,
                at_z(k),
            )
        xs[a, blk(z), cols] = r1p[a, blk(z), cols]

    def other(index):
        return pl.ds(pl.multiple_of(rows + index * block, block), block)

    def forward(a, j, which):
        lo, width = chunks[j]
        cols = pl.ds(lo, width)
        for k in which:
            zs = z_from(k)
            if k:
                copies.arrived(
                    xs.at[a, blk(zs), cols], st2 + (2 * a + j) * (planes - 1) + k - 1, from_z(k)
                )
            copies.start(
                xs.at[a, blk(zs), cols], xs.at[a, other(zs), cols], fwd + (2 * a + j) * planes + k, token_y
            )

    def forwarded(a):
        for j, (lo, width) in enumerate(chunks):
            for k in [0] + z_order:
                copies.arrived(
                    xs.at[a, other(z_from(k)), pl.ds(lo, width)], fwd + (2 * a + j) * planes + k, token_y
                )

    loads[0].wait()
    gather(0, 0)
    gather(0, 1)
    loads[1].wait()
    gather(1, 0)
    gather(1, 1)
    plane_stage(0, 0)
    plane_stage(0, 1)
    every = [0] + z_order
    first, last = every[: planes // 2], every[planes // 2 :]
    forward(0, 0, every)
    plane_stage(1, 0)
    forward(0, 1, every)
    plane_stage(1, 1)

    mine = c * 2 * part
    theirs = (1 - c) * 2 * part
    rs1 = copies.slots(4)
    rs2 = copies.slots(4)

    def rows_at(t, offset, size):
        return pl.ds(pl.multiple_of(t * rows + offset, part), size)

    def project(a, t, offset, kinds, dst):
        left = xs.at[a, rows_at(t, offset, 2 * part), :]

        def step(i, carry):
            w, b = kinds[0] + i // 2, lax.rem(i, 2)
            got = lax.dot_general(
                left[...],
                wv[w, pl.ds(pl.multiple_of(b * units, units), units), :],
                NT,
                preferred_element_type=F32,
            )
            dst[:, pl.ds(pl.multiple_of(i * units, units), units)] = got.astype(dst.dtype)
            return carry

        lax.fori_loop(0, 2 * len(kinds), step, 0)

    def to_core(a, t, kinds, send, recv, keep, slot):
        project(a, t, theirs, kinds, send.at[t])
        copies.start(send.at[t], recv.at[t], slot + t, at_u(1))
        project(a, t, mine, kinds, keep.at[t])

    def to_chip(t, recv, keep, send2, recv2, slot, slot2):
        copies.arrived(recv.at[t], slot + t, at_u(1))
        away = pl.ds(pl.multiple_of((1 - bx) * part, part), part)
        send2[t] = (keep[t, away, :] + recv[t, away, :].astype(F32)).astype(BF)
        copies.start(send2.at[t], recv2.at[t], slot2 + t, at_u(2))

    def summed(t, recv, keep, recv2, slot2):
        copies.arrived(recv2.at[t], slot2 + t, at_u(2))
        here = pl.ds(pl.multiple_of(bx * part, part), part)
        return keep[t, here, :] + recv[t, here, :].astype(F32) + recv2[t].astype(F32)

    def piece(t, core, side):
        return rows_at(t, core * 2 * part + side * part, part)

    def share(ref, t, slot):
        own = ref.at[piece(t, c, bx)]
        copies.start(own, own, slot, at_u(2))
        copies.start(own, own, slot + 1, at_u(1))

    def relay(ref, t, slot):
        theirs_too = ref.at[piece(t, c, 1 - bx)]
        copies.arrived(theirs_too, slot, at_u(2))
        copies.start(theirs_too, theirs_too, slot + 2, at_u(1))

    def gathered(ref, t, slot):
        copies.arrived(ref.at[piece(t, 1 - c, bx)], slot + 1, at_u(1))
        copies.arrived(ref.at[piece(t, 1 - c, 1 - bx)], slot + 2, at_u(1))

    ag = copies.slots(12)
    width_h = 2 * units

    def hidden(t):
        both = summed(t, gu_recv, gu_keep, gu_recv2, rs1 * 0 + rs2)
        gu_own[t] = both
        gate, up = both[:, :width_h], both[:, width_h:]
        hid[piece(t, c, bx)] = (gate * jax.nn.sigmoid(gate) * up).astype(BF)
        share(hid, t, ag + 3 * t)

    def gradients(t):
        back = summed(t, bk_recv, bk_keep, bk_recv2, rs2 + 2)
        gate, up = gu_own[t, :, :width_h], gu_own[t, :, width_h:]
        logistic = jax.nn.sigmoid(gate)
        own = piece(t, c, bx)
        dgu[own, :width_h] = (back * up * logistic * (1.0 + gate * (1.0 - logistic))).astype(BF)
        dgu[own, width_h:] = (back * (gate * logistic)).astype(BF)
        share(dgu, t, ag + 6 + 3 * t)

    for w in (0, 1):
        loads[2 + w].wait()
        copies.arrived(wv.at[w, pl.ds(units, units)], w_slot + w, weight_y)
    to_core(0, 0, (0, 1), gu_send, gu_recv, gu_keep, rs1)
    forward(1, 0, first)
    forwarded(0)
    to_core(0, 1, (0, 1), gu_send, gu_recv, gu_keep, rs1)
    to_chip(0, gu_recv, gu_keep, gu_send2, gu_recv2, rs1, rs2)
    to_chip(1, gu_recv, gu_keep, gu_send2, gu_recv2, rs1, rs2)
    forward(1, 0, last)
    hidden(0)
    hidden(1)
    forward(1, 1, first)
    relay(hid, 0, ag)
    relay(hid, 1, ag + 3)
    forward(1, 1, last)

    loads[4].wait()
    copies.arrived(wv.at[2, pl.ds(units, units)], w_slot + 2, weight_y)
    to_core(1, 0, (2,), bk_send, bk_recv, bk_keep, rs1 + 2)
    forwarded(1)
    to_core(1, 1, (2,), bk_send, bk_recv, bk_keep, rs1 + 2)
    to_chip(0, bk_recv, bk_keep, bk_send2, bk_recv2, rs1 + 2, rs2 + 2)
    to_chip(1, bk_recv, bk_keep, bk_send2, bk_recv2, rs1 + 2, rs2 + 2)

    gr = copies.slots(3)
    span = quarter // 7

    def grad_term(w, b, a, left, at):
        dt[...] = left[:, pl.ds(at + b * units, units)].T

        def step(i, carry):
            cols = pl.ds(pl.multiple_of(i * span, span), span)
            got = lax.dot_general(dt[...], xs[a, :, cols], NN, preferred_element_type=F32)
            gterm[b, w, :, cols] = got.astype(BF)
            return carry

        lax.fori_loop(0, 7, step, 0)
        if b:
            copies.start(gterm.at[1, w], grecv.at[w], gr + w, weight_y)

    gathered(hid, 0, ag)
    gathered(hid, 1, ag + 3)
    grad_term(2, 1, 1, hid, 0)
    gradients(0)
    gradients(1)
    relay(dgu, 0, ag + 6)
    relay(dgu, 1, ag + 9)
    gathered(dgu, 1, ag + 9)
    gathered(dgu, 0, ag + 6)

    parts = pieces(quarter)
    dxy = copies.slots(4)
    dxz = copies.slots(4 * (planes - 1))
    dxu = copies.slots(4 * (plane - 1))

    def dx_term(t, i):
        lo, width = parts[i]
        cols = pl.ds(lo, width)
        at = pl.ds(t * rows, rows)
        got = lax.dot_general(dgu[at, :width_h], wv[0, :, cols], NN, preferred_element_type=F32)
        return got + lax.dot_general(dgu[at, width_h:], wv[1, :, cols], NN, preferred_element_type=F32)

    def dx_out(i):
        lo, width = parts[i]
        cols = pl.ds(lo, width)
        dx_send[:, cols] = dx_term(1, i).astype(BF)
        copies.start(dx_send.at[:, cols], dx_recv.at[:, cols], dxy + i, token_y)

    def dx_here(i):
        lo, width = parts[i]
        dx_own[:, pl.ds(lo, width)] = dx_term(0, i)

    def dx_z(i):
        lo, width = parts[i]
        cols = pl.ds(lo, width)
        copies.arrived(dx_recv.at[:, cols], dxy + i, token_y)
        dxs[:, cols] = (dx_own[:, cols] + dx_recv[:, cols].astype(F32)).astype(BF)
        for k in z_order:
            copies.start(
                dxs.at[blk(z_to(k)), cols], rz.at[blk(z), cols], dxz + i * (planes - 1) + k - 1, at_z(k)
            )
        rz[blk(z), cols] = dxs[blk(z), cols]

    def dx_u(i):
        lo, width = parts[i]
        cols = pl.ds(lo, width)
        for k in z_order:
            copies.arrived(rz.at[blk(z_from(k)), cols], dxz + i * (planes - 1) + k - 1, from_z(k))
        rzp[:, cols] = lax.dot_general(
            perm_t_ref[...], rz[:, cols], NN, preferred_element_type=F32
        ).astype(BF)
        for k in u_order:
            copies.start(
                rzp.at[blk(in_plane(k)), cols], ret.at[u, :, cols], dxu + i * (plane - 1) + k - 1, at_u(k)
            )
        ret[u, :, cols] = rzp[blk(u), cols]

    def dx_back(i):
        lo, width = parts[i]
        cols = pl.ds(lo, width)
        for k in u_order:
            copies.arrived(ret.at[in_plane(k), :, cols], dxu + i * (plane - 1) + k - 1, at_u(k))
        for q in range(GROUP):
            total = None
            for h in range(plane // GROUP):
                got = lax.dot_general(
                    sel_t_ref[h], ret[h * GROUP + q, :, cols], NN, preferred_element_type=F32
                )
                total = got if total is None else total + got
            out_ref[:, pl.ds(q * quarter + lo, width)] = total.astype(BF)

    dx_out(0)
    grad_term(0, 1, 0, dgu, 0)
    dx_out(1)
    grad_term(1, 1, 0, dgu, width_h)
    dx_out(2)
    dx_out(3)
    for i in range(4):
        dx_here(i)
    dx_z(0)
    grad_term(0, 0, 0, dgu, 0)
    dx_z(1)
    dx_u(0)
    grad_term(1, 0, 0, dgu, width_h)
    dx_z(2)
    dx_u(1)
    grad_term(2, 0, 1, hid, 0)
    dx_z(3)
    dx_u(2)
    dx_u(3)
    for i in range(4):
        dx_back(i)

    for w in (2, 0, 1):
        copies.arrived(grecv.at[w], gr + w, weight_y)
        gout_ref[w] = (gterm[0, w].astype(F32) + grecv[w].astype(F32)).astype(BF)
    copies.drain()


def slot_choice(expert_ids, route_weight, order, capacity):
    experts = order.shape[0]
    ids = expert_ids.reshape(-1)
    count = ids.shape[0]
    same = (ids[:, None] == ids[None, :]) & (jnp.arange(count)[None, :] < jnp.arange(count)[:, None])
    ranks = jnp.sum(same.astype(jnp.int32), axis=1)
    expert_of_slot = jnp.repeat(order, capacity)
    rank_of_slot = jnp.tile(jnp.arange(capacity, dtype=jnp.int32), experts)
    match = (ids[None, :] == expert_of_slot[:, None]) & (ranks[None, :] == rank_of_slot[:, None])
    weight = jnp.sum(jnp.where(match, route_weight.reshape(-1)[None, :], 0.0), axis=1, keepdims=True)
    return match, weight


def body(planes, plane, capacity, tokens, out_grad, route_weight, expert_ids, w_gate, w_up, w_down):
    count, width = tokens.shape
    quarter = width // GROUP
    units = w_gate.shape[0]
    block = planes * capacity
    rows = plane * block
    part = rows // 4
    sides = plane // GROUP
    order = jnp.arange(planes * sides, dtype=jnp.int32).reshape(planes, sides).T.reshape(-1)
    match, weight = slot_choice(expert_ids, route_weight, order, capacity)
    sel = match.astype(BF)
    sel_t = sel.reshape(sides, block, count).transpose(0, 2, 1)
    at = jnp.arange(rows, dtype=jnp.int32)
    zi, ui, si = at // (plane * capacity), at // capacity % plane, at % capacity
    perm = (at[None, :] == (ui * block + zi * capacity + si)[:, None]).astype(BF)
    perm_t = (at[:, None] == (ui * block + zi * capacity + si)[None, :]).astype(BF)
    vmem = pl.BlockSpec(memory_space=pltpu.VMEM)
    hbm = pl.BlockSpec(memory_space=pl.ANY)
    sems = semaphores(planes, plane)
    in_grad, grads = pl.pallas_call(
        functools.partial(kernel, planes, plane, capacity),
        out_shape=(
            jax.ShapeDtypeStruct((count, width), BF),
            jax.ShapeDtypeStruct((3, units, quarter), BF),
        ),
        in_specs=[vmem] * 5 + [hbm] * 5,
        out_specs=(vmem, vmem),
        scratch_shapes=[
            pltpu.VMEM((2, count, width), BF),
            pltpu.VMEM((2, plane, block, quarter), BF),
            pltpu.VMEM((2, rows, quarter), BF),
            pltpu.VMEM((2, rows, quarter), BF),
            pltpu.VMEM((2, 2 * rows, quarter), BF),
            pltpu.VMEM((3, 2 * units, quarter), BF),
            pltpu.VMEM((2, 2 * part, 4 * units), BF),
            pltpu.VMEM((2, 2 * part, 4 * units), BF),
            pltpu.VMEM((2, 2 * part, 4 * units), F32),
            pltpu.VMEM((2, part, 4 * units), BF),
            pltpu.VMEM((2, part, 4 * units), BF),
            pltpu.VMEM((2, 2 * part, 2 * units), BF),
            pltpu.VMEM((2, 2 * part, 2 * units), BF),
            pltpu.VMEM((2, 2 * part, 2 * units), F32),
            pltpu.VMEM((2, part, 2 * units), BF),
            pltpu.VMEM((2, part, 2 * units), BF),
            pltpu.VMEM((2, part, 4 * units), F32),
            pltpu.VMEM((2 * rows, 2 * units), BF),
            pltpu.VMEM((2 * rows, 4 * units), BF),
            pltpu.VMEM((units, 2 * rows), BF),
            pltpu.VMEM((2, 3, units, quarter), BF),
            pltpu.VMEM((3, units, quarter), BF),
            pltpu.VMEM((rows, quarter), BF),
            pltpu.VMEM((rows, quarter), BF),
            pltpu.VMEM((rows, quarter), F32),
            pltpu.VMEM((rows, quarter), BF),
            pltpu.VMEM((rows, quarter), BF),
            pltpu.VMEM((rows, quarter), BF),
            pltpu.VMEM((plane, block, quarter), BF),
            pltpu.SemaphoreType.DMA((5,)),
            pltpu.SemaphoreType.DMA((sems,)),
            pltpu.SemaphoreType.DMA((sems,)),
        ],
        compiler_params=pltpu.CompilerParams(
            collective_id=0, has_side_effects=True, vmem_limit_bytes=63 * 1024 * 1024
        ),
        name="expert_backward",
    )(sel, sel_t, weight, perm, perm_t, tokens, out_grad, w_gate, w_up, w_down)
    return in_grad, grads[0], grads[1], grads[2]


def solution(mesh):
    tokens = P(("dp", "ep"), None)
    weights = P("dp", "ep")
    planes = mesh.shape["ep"] // PLANE
    return jax.shard_map(
        functools.partial(body, planes, PLANE, CAP),
        mesh=mesh,
        in_specs=(tokens, tokens, tokens, tokens, weights, weights, weights),
        out_specs=(tokens, weights, weights, weights),
        check_vma=False,
    )
```

```python
import functools

import jax
import jax.numpy as jnp
from jax import lax
from jax.experimental import pallas as pl
from jax.experimental.pallas import tpu as pltpu
from jax.sharding import PartitionSpec as P

D = 7168
GROUP = 4
CAP = 6
PLANE = 8
NT = (((1,), (1,)), ((), ()))
NN = (((1,), (0,)), ((), ()))
MESH = pl.DeviceIdType.MESH
BF = jnp.bfloat16
F32 = jnp.float32


def scope(stage):
    @functools.wraps(stage)
    def named(*args):
        tag = "_".join(str(a) for a in args if isinstance(a, int))
        with jax.named_scope(f"{stage.__name__}_{tag}"):
            return stage(*args)

    return named


class Copies:
    def __init__(self, send, recv):
        self.send, self.recv, self.sends, self.recvs, self.open = send, recv, 0, 0, []

    def sender(self, whole):
        self.open.append((whole, self.sends))
        self.sends += 1
        return self.sends - 1

    def slots(self, count):
        self.recvs += count
        return self.recvs - count

    def make(self, src, dst, sent, slot, device):
        return pltpu.make_async_remote_copy(
            src_ref=src,
            dst_ref=dst,
            send_sem=self.send.at[sent],
            recv_sem=self.recv.at[slot],
            device_id=device,
            device_id_type=MESH,
        )

    def start(self, src, dst, sent, slot, device):
        self.make(src, dst, sent, slot, device).start()

    def arrived(self, whole, slot, device):
        self.make(whole, whole, 0, slot, device).wait_recv()

    def drain(self, device):
        for whole, sent in self.open:
            self.make(whole, whole, sent, 0, device).wait_send()


def cut(width, sizes):
    unit, at, out = width // 14, 0, []
    for size in sizes:
        out.append((at, size * unit))
        at += size * unit
    return out


IN_CUTS = ((1, 2, 4, 4, 3), (4, 4, 4, 2))
OUT_CUT = (1, 3, 3, 3, 2, 1, 1)
GRAD_CUT = (4, 4, 4, 2)
SENDERS = 15


def receivers(planes):
    chunks = len(IN_CUTS[0]) + len(IN_CUTS[1])
    return chunks * (2 + planes // 2) + 3 * len(OUT_CUT) + 3 + 6 + 6 + 1 + 2 + 3


def slot_tables(planes, plane, cap, ids_ref, rw_ref, sel_ref, sel_t_ref, scale_ref, perm_ref, perm_t_ref):
    count = ids_ref.shape[1]
    block, rows, sides = planes * cap, perm_ref.shape[0], plane // GROUP
    by_col = jnp.broadcast_to(ids_ref[...].astype(F32), (count, count))
    by_row = by_col.T
    i = lax.broadcasted_iota(jnp.int32, (count, count), 0)
    j = lax.broadcasted_iota(jnp.int32, (count, count), 1)
    same = by_col == by_row
    rank_col = jnp.sum(jnp.where(same & (i < j), 1.0, 0.0), axis=0, keepdims=True)
    rank_row = jnp.sum(jnp.where(same & (j < i), 1.0, 0.0), axis=1, keepdims=True)

    def wanted(shape, axis, side_rows):
        at = lax.broadcasted_iota(jnp.int32, shape, axis)
        side, at = at // side_rows, lax.rem(at, side_rows)
        expert = at // cap * sides + side
        return expert.astype(F32), lax.rem(at, cap).astype(F32)

    expert, rank = wanted((sides * block, count), 0, block)
    match = (by_col[:1] == expert) & (rank_col == rank)
    sel_ref[...] = jnp.where(match, 1.0, 0.0).astype(BF)
    scale_ref[...] = jnp.sum(jnp.where(match, rw_ref[...], 0.0), axis=1, keepdims=True)
    expert, rank = wanted((count, block), 1, block)
    for side in range(sides):
        match = (by_row[:, :1] == expert + float(side)) & (rank_row == rank)
        sel_t_ref[side] = jnp.where(match, 1.0, 0.0).astype(BF)

    def source(shape, axis):
        at = lax.broadcasted_iota(jnp.int32, shape, axis)
        zi, rest = at // (plane * cap), lax.rem(at, plane * cap)
        return rest // cap * block + zi * cap + lax.rem(rest, cap)

    i = lax.broadcasted_iota(jnp.int32, (rows, rows), 0)
    j = lax.broadcasted_iota(jnp.int32, (rows, rows), 1)
    perm_ref[...] = jnp.where(source((rows, 1), 0) == j, 1.0, 0.0).astype(BF)
    perm_t_ref[...] = jnp.where(source((1, rows), 1) == i, 1.0, 0.0).astype(BF)


def kernel(
    planes, plane, cap,
    ids_ref, rw_ref, tok_hbm, grad_hbm, wg_hbm, wu_hbm, wd_hbm,
    out_ref, og_ref, ou_ref, od_ref,
    sel_ref, sel_t_ref, scale_ref, perm_ref, perm_t_ref, raw,
    send1, r1, r1p, xs, wgu, wdn, acc, core_out, core_in, chip_out, chip_in,
    hid, hid_t, dgu, dgu_t, gterm, gown, grecv, dx_send, dx_recv, dx_own, dxs, rz, rzp, ret,
    local_sem, send_sem, recv_sem,
):
    quarter = xs.shape[2]
    block = planes * cap
    rows = plane * block
    half = rows // 2
    units = hid.shape[1] // 2
    r = lax.axis_index("dp")
    ep = lax.axis_index("ep")
    z = ep // plane
    u = lax.rem(ep, plane)
    c = lax.rem(u, 2)
    copies = Copies(send_sem, recv_sem)

    def in_plane(k):
        out = u
        for bit in range(3):
            if k >> bit & 1:
                out = out + (1 << bit) * (1 - 2 * lax.rem(u // (1 << bit), 2))
        return out

    def at_u(k):
        return (r, z * plane + in_plane(k))

    def z_to(k):
        return lax.rem(z + k, planes)

    def z_from(k):
        return lax.rem(z + planes - k, planes)

    def at_z(k):
        return (r, z_to(k) * plane + u)

    def from_z(k):
        return (r, z_from(k) * plane + u)

    def blk(index):
        return pl.ds(pl.multiple_of(index * block, block), block)

    def other(index):
        return pl.ds(pl.multiple_of(rows + index * block, block), block)

    reach = [sorted({k, planes - k}) for k in range(1, planes // 2 + 1)]
    z_order = [k for group in reach for k in group]
    u_order = [k for k in (4, 5, 2, 3, 6, 7, 1) if k < plane]
    token_y, weight_y = (r + 1 - 2 * lax.rem(r, 2), ep), (3 - r, ep)

    own_w = (
        (wg_hbm, wgu.at[pl.ds(0, units)], wgu.at[pl.ds(2 * units, units)]),
        (wu_hbm, wgu.at[pl.ds(units, units)], wgu.at[pl.ds(3 * units, units)]),
        (wd_hbm, wdn.at[pl.ds(0, units)], wdn.at[pl.ds(units, units)]),
    )
    loads = [
        pltpu.make_async_copy(tok_hbm, raw.at[0], local_sem.at[0]),
        pltpu.make_async_copy(grad_hbm, raw.at[1], local_sem.at[1]),
    ]
    for w, (ref, here, _) in enumerate(own_w):
        loads.append(pltpu.make_async_copy(ref, here, local_sem.at[2 + w]))
    loads[0].start()

    barrier = pltpu.get_barrier_semaphore()
    partners = [at_u(k) for k in u_order] + [at_z(k) for k in z_order] + [token_y, weight_y]
    for device in partners:
        pl.semaphore_signal(barrier, inc=1, device_id=device, device_id_type=MESH)

    with jax.named_scope("tables"):
        slot_tables(
            planes, plane, cap, ids_ref, rw_ref, sel_ref, sel_t_ref, scale_ref, perm_ref, perm_t_ref
        )
    w_slot = copies.slots(3)
    w_sent = copies.sender(wgu.at[pl.ds(0, 3 * units)])

    @scope
    def weight_here(w):
        loads[2 + w].wait()

    @scope
    def weight(w):
        copies.arrived(own_w[w][2], w_slot + w, weight_y)

    chunks = [cut(quarter, sizes) for sizes in IN_CUTS]
    index = [[0, 1, 2, 3, 4], [5, 6, 7, 8]]
    total = len(IN_CUTS[0]) + len(IN_CUTS[1])
    st1, st2, fwd = copies.slots(total), copies.slots(total * len(reach)), copies.slots(total)
    st1_sent = [copies.sender(r1p.at[a, pl.ds(0, rows - block)]) for a in range(2)]
    st2_sent = [copies.sender(r1p.at[a, pl.ds(0, rows - rows // planes)]) for a in range(2)]
    fwd_sent = [copies.sender(xs.at[a, pl.ds(0, rows)]) for a in range(2)]

    @scope
    def gather(a, j):
        lo, width = chunks[a][j]
        cols = pl.ds(lo, width)
        for q in range(GROUP):
            got = lax.dot_general(
                sel_ref[...], raw[a, :, pl.ds(q * quarter + lo, width)], NN, preferred_element_type=F32
            )
            if a:
                got = got * scale_ref[...]
            got = got.astype(BF)
            for h in range(plane // GROUP):
                send1[a, h * GROUP + q, :, cols] = got[h * block : (h + 1) * block]
        r1[a, blk(u), cols] = send1[a, u, :, cols]

    @scope
    def to_plane(a, j):
        cols = pl.ds(*chunks[a][j])
        for k in u_order:
            copies.start(
                send1.at[a, in_plane(k), :, cols],
                r1.at[a, blk(u), cols],
                st1_sent[a],
                st1 + index[a][j],
                at_u(k),
            )

    @scope
    def plane_stage(a, j):
        cols = pl.ds(*chunks[a][j])
        copies.arrived(r1.at[a, pl.ds(0, rows - block), cols], st1 + index[a][j], at_u(1))
        r1p[a, :, cols] = lax.dot_general(
            perm_ref[...], r1[a, :, cols], NN, preferred_element_type=F32
        ).astype(BF)
        for g, group in enumerate(reach):
            for k in group:
                copies.start(
                    r1p.at[a, blk(z_to(k)), cols],
                    xs.at[a, blk(z), cols],
                    st2_sent[a],
                    st2 + index[a][j] * len(reach) + g,
                    at_z(k),
                )
        xs[a, blk(z), cols] = r1p[a, blk(z), cols]

    @scope
    def forward(a, j, g0, g1):
        cols = pl.ds(*chunks[a][j])
        for g in range(g0, min(g1, len(reach))):
            if g == 0:
                pass_on(a, j, 0)
            copies.arrived(
                xs.at[a, pl.ds(0, len(reach[g]) * block), cols],
                st2 + index[a][j] * len(reach) + g,
                at_z(1),
            )
            for k in reach[g]:
                pass_on(a, j, k)

    def pass_on(a, j, k):
        cols = pl.ds(*chunks[a][j])
        zs = z_from(k)
        copies.start(
            xs.at[a, blk(zs), cols], xs.at[a, other(zs), cols], fwd_sent[a], fwd + index[a][j], token_y
        )

    @scope
    def forwarded(a, j):
        cols = pl.ds(*chunks[a][j])
        copies.arrived(xs.at[a, pl.ds(rows, rows), cols], fwd + index[a][j], token_y)

    mine = lambda t: pl.ds(pl.multiple_of(t * rows + c * half, half), half)
    theirs = lambda t: pl.ds(pl.multiple_of(t * rows + (1 - c) * half, half), half)
    core = copies.slots(6)
    chip = copies.slots(6)
    share_h, share_d = copies.slots(1), copies.slots(2)
    core_sent, chip_sent = copies.sender(core_out), copies.sender(chip_out)
    h_sent, d_sent = copies.sender(hid.at[pl.ds(0, rows)]), copies.sender(dgu.at[pl.ds(0, rows)])
    span = 2 * units

    def project(left, weights, t, g, cols, add):
        at = pl.ds(t * rows, rows)

        def step(b, carry):
            got = lax.dot_general(
                left[at, cols],
                weights[pl.ds(pl.multiple_of(b * units, units), units), cols],
                NT,
                preferred_element_type=F32,
            )
            to = pl.ds(pl.multiple_of(g * span + b * units, units), units)
            acc[at, to] = acc[at, to] + got if add else got
            return carry

        lax.fori_loop(0, 2, step, 0)

    @scope
    def gate_up(t, b):
        project(xs.at[0], wgu.at[pl.ds(b * span, span)], t, b, pl.ds(0, quarter), False)

    @scope
    def back(t, j0, j1):
        lo = chunks[1][j0][0]
        width = sum(chunks[1][j1]) - lo
        project(xs.at[1], wdn, t, 2, pl.ds(lo, width), j0 > 0)

    @scope
    def to_core(t, g):
        cols = pl.ds(g * span, span)
        core_out[t, :, cols] = acc[theirs(t), cols].astype(BF)
        copies.start(core_out.at[t, :, cols], core_in.at[t, :, cols], core_sent, core + 3 * t + g, at_u(1))

    @scope
    def to_chip(t, g):
        cols = pl.ds(g * span, span)
        copies.arrived(core_in.at[t, :, cols], core + 3 * t + g, at_u(1))
        pair = acc[mine(t), cols] + core_in[t, :, cols].astype(F32)
        acc[mine(t), cols] = pair
        chip_out[t, :, cols] = pair.astype(BF)
        copies.start(chip_out.at[t, :, cols], chip_in.at[t, :, cols], chip_sent, chip + 3 * t + g, at_u(2))

    def summed(t, g):
        cols = pl.ds(g * span, span)
        copies.arrived(chip_in.at[t, :, cols], chip + 3 * t + g, at_u(2))
        return acc[mine(t), cols] + chip_in[t, :, cols].astype(F32)

    @scope
    def hidden(t, b):
        both = summed(t, b)
        acc[mine(t), pl.ds(b * span, span)] = both
        gate, up = both[:, :units], both[:, units:]
        at = hid.at[mine(t), pl.ds(b * units, units)]
        at[...] = (gate * jax.nn.sigmoid(gate) * up).astype(BF)
        copies.start(at, at, h_sent, share_h, at_u(1))

    @scope
    def gradients(t):
        both = summed(t, 2)
        for b in range(2):
            gate = acc[mine(t), pl.ds(b * span, units)]
            up = acc[mine(t), pl.ds(b * span + units, units)]
            grad = both[:, b * units : (b + 1) * units]
            logistic = jax.nn.sigmoid(gate)
            dgu[mine(t), pl.ds(b * span, units)] = (
                grad * up * logistic * (1.0 + gate * (1.0 - logistic))
            ).astype(BF)
            dgu[mine(t), pl.ds(b * span + units, units)] = (grad * (gate * logistic)).astype(BF)
        at = dgu.at[mine(t)]
        copies.start(at, at, d_sent, share_d + t, at_u(1))

    @scope
    def hidden_here():
        copies.arrived(hid.at[pl.ds(0, rows)], share_h, at_u(1))

    @scope
    def gradients_here(t):
        copies.arrived(dgu.at[theirs(t)], share_d + t, at_u(1))

    grad_cut = cut(quarter, GRAD_CUT)
    gr = copies.slots(3)
    gr_sent = copies.sender(gterm)

    @scope
    def flip_hidden():
        hid_t[...] = hid[...].T

    @scope
    def flip_gradients(b):
        dgu_t[pl.ds(b * span, span)] = dgu[:, pl.ds(b * span, span)].T

    @scope
    def down_out(i):
        cols = pl.ds(*grad_cut[i])
        gterm[2, :, cols] = lax.dot_general(
            hid_t[pl.ds(units, units)], xs[1, :, cols], NN, preferred_element_type=F32
        ).astype(BF)
        copies.start(gterm.at[2, :, cols], grecv.at[2, :, cols], gr_sent, gr + 2, weight_y)

    @scope
    def gate_up_out(i):
        cols = pl.ds(*grad_cut[i])
        for w in range(2):
            gterm[w, :, cols] = lax.dot_general(
                dgu_t[pl.ds(span + w * units, units)], xs[0, :, cols], NN, preferred_element_type=F32
            ).astype(BF)
            copies.start(gterm.at[w, :, cols], grecv.at[w, :, cols], gr_sent, gr + w, weight_y)

    @scope
    def term_here(w):
        left = hid_t.at[pl.ds(0, units)] if w == 2 else dgu_t.at[pl.ds(w * units, units)]
        for lo, width in grad_cut:
            cols = pl.ds(lo, width)
            gown[w, :, cols] = lax.dot_general(
                left[...], xs[w // 2, :, cols], NN, preferred_element_type=F32
            ).astype(BF)

    @scope
    def grad_out(w, ref):
        copies.arrived(grecv.at[w], gr + w, weight_y)
        ref[...] = (gown[w].astype(F32) + grecv[w].astype(F32)).astype(BF)

    parts = cut(quarter, OUT_CUT)
    dxy = copies.slots(len(parts))
    dxz, dxu = copies.slots(len(parts)), copies.slots(len(parts))
    dxy_sent = copies.sender(dx_send)
    dxz_sent = copies.sender(dxs.at[pl.ds(0, rows - rows // planes)])
    dxu_sent = copies.sender(dxs.at[pl.ds(0, rows - block)])

    def dx_term(t, cols):
        return lax.dot_general(
            dgu[pl.ds(t * rows, rows)], wgu[:, cols], NN, preferred_element_type=F32
        )

    @scope
    def dx_out(i):
        cols = pl.ds(*parts[i])
        dx_send[:, cols] = dx_term(1, cols).astype(BF)
        copies.start(dx_send.at[:, cols], dx_recv.at[:, cols], dxy_sent, dxy + i, token_y)

    @scope
    def dx_here(i):
        cols = pl.ds(*parts[i])
        dx_own[:, cols] = dx_term(0, cols)

    @scope
    def dx_z(i):
        cols = pl.ds(*parts[i])
        copies.arrived(dx_recv.at[:, cols], dxy + i, token_y)
        dxs[:, cols] = (dx_own[:, cols] + dx_recv[:, cols].astype(F32)).astype(BF)
        for k in reversed(z_order):
            copies.start(
                dxs.at[blk(z_to(k)), cols], rz.at[blk(z), cols], dxz_sent, dxz + i, at_z(k)
            )
        rz[blk(z), cols] = dxs[blk(z), cols]

    @scope
    def dx_u(i):
        cols = pl.ds(*parts[i])
        copies.arrived(rz.at[pl.ds(0, rows - rows // planes), cols], dxz + i, at_z(1))
        rzp[:, cols] = lax.dot_general(
            perm_t_ref[...], rz[:, cols], NN, preferred_element_type=F32
        ).astype(BF)
        for k in u_order:
            copies.start(
                rzp.at[blk(in_plane(k)), cols], ret.at[u, :, cols], dxu_sent, dxu + i, at_u(k)
            )
        ret[u, :, cols] = rzp[blk(u), cols]

    @scope
    def dx_back(i):
        lo, width = parts[i]
        cols = pl.ds(lo, width)
        copies.arrived(rz.at[pl.ds(0, rows - block), cols], dxu + i, at_u(1))
        for q in range(GROUP):
            total = None
            for h in range(plane // GROUP):
                got = lax.dot_general(
                    sel_t_ref[h], ret[h * GROUP + q, :, cols], NN, preferred_element_type=F32
                )
                total = got if total is None else total + got
            out_ref[:, pl.ds(q * quarter + lo, width)] = total.astype(BF)

    loads[0].wait()
    for load in loads[1:]:
        load.start()
    gather(0, 0)
    gather(0, 1)
    with jax.named_scope("barrier"):
        pl.semaphore_wait(barrier, len(partners))
    to_plane(0, 0)
    for w, (ref, _, there) in enumerate(own_w):
        copies.start(ref, there, w_sent, w_slot + w, weight_y)
    to_plane(0, 1)
    for j in range(2, 5):
        gather(0, j)
        to_plane(0, j)
    loads[1].wait()
    for j in range(4):
        gather(1, j)
        to_plane(1, j)
    plane_stage(0, 0)
    plane_stage(0, 1)
    forward(0, 0, 0, 4)
    plane_stage(0, 2)
    forward(0, 1, 0, 4)
    plane_stage(0, 3)
    forward(0, 2, 0, 4)
    plane_stage(0, 4)
    forward(0, 3, 0, 4)
    plane_stage(1, 0)
    forward(0, 4, 0, 4)
    plane_stage(1, 1)
    weight_here(0)
    weight_here(1)
    gate_up(0, 0)
    to_core(0, 0)
    forward(1, 0, 0, 1)
    for j in range(5):
        forwarded(0, j)
    gate_up(1, 0)
    to_core(1, 0)
    to_chip(0, 0)
    forward(1, 0, 1, 2)
    weight(0)
    weight(1)
    gate_up(0, 1)
    to_core(0, 1)
    to_chip(1, 0)
    gate_up(1, 1)
    to_core(1, 1)
    forward(1, 0, 2, 4)
    to_chip(0, 1)
    plane_stage(1, 2)
    to_chip(1, 1)
    plane_stage(1, 3)
    forward(1, 1, 0, 1)
    hidden(0, 0)
    forward(1, 1, 1, 4)
    hidden(1, 0)
    forward(1, 2, 0, 2)
    hidden(0, 1)
    forward(1, 2, 2, 3)
    hidden(1, 1)
    forward(1, 2, 3, 4)
    hidden_here()
    flip_hidden()
    forwarded(1, 0)
    down_out(0)
    forward(1, 3, 0, 1)
    forwarded(1, 1)
    down_out(1)
    weight_here(2)
    weight(2)
    forward(1, 3, 1, 2)
    back(0, 0, 2)
    forward(1, 3, 2, 3)
    back(1, 0, 1)
    forward(1, 3, 3, 4)
    back(0, 3, 3)
    to_core(0, 2)
    forwarded(1, 2)
    back(1, 2, 2)
    to_chip(0, 2)
    forwarded(1, 3)
    back(1, 3, 3)
    to_core(1, 2)
    down_out(2)
    to_chip(1, 2)
    gradients(0)
    down_out(3)
    gradients(1)
    gradients_here(0)
    gradients_here(1)
    dx_out(0)
    flip_gradients(1)
    gate_up_out(0)
    dx_out(1)
    gate_up_out(1)
    dx_out(2)
    dx_here(0)
    dx_z(0)
    dx_out(3)
    gate_up_out(2)
    dx_out(4)
    gate_up_out(3)
    dx_out(5)
    dx_out(6)
    dx_here(1)
    dx_here(2)
    dx_z(1)
    dx_u(0)
    for i in range(3, 7):
        dx_here(i)
    flip_gradients(0)
    dx_z(2)
    dx_u(1)
    dx_back(0)
    term_here(2)
    dx_z(3)
    dx_u(2)
    dx_back(1)
    dx_z(4)
    term_here(0)
    dx_z(5)
    dx_u(3)
    dx_back(2)
    dx_z(6)
    term_here(1)
    dx_u(4)
    grad_out(2, od_ref)
    dx_u(5)
    dx_back(3)
    dx_u(6)
    dx_back(4)
    dx_back(5)
    dx_back(6)
    grad_out(0, og_ref)
    grad_out(1, ou_ref)
    with jax.named_scope("drain"):
        copies.drain(token_y)
    assert (copies.sends, copies.recvs) == (SENDERS, receivers(planes))


def store(*refs):
    sems = refs[-1]
    moves = [pltpu.make_async_copy(refs[i], refs[4 + i], sems.at[i]) for i in range(4)]
    for move in moves:
        move.start()
    for move in moves:
        move.wait()


def body(planes, plane, capacity, tokens, out_grad, route_weight, expert_ids, w_gate, w_up, w_down):
    count, width = tokens.shape
    quarter = width // GROUP
    units = w_gate.shape[0]
    block = planes * capacity
    rows = plane * block
    half = rows // 2
    sides = plane // GROUP
    vmem = pl.BlockSpec(memory_space=pltpu.VMEM)
    hbm = pl.BlockSpec(memory_space=pl.ANY)
    results = pl.pallas_call(
        functools.partial(kernel, planes, plane, capacity),
        out_shape=(
            pltpu.VMEM((count, width), BF),
            pltpu.VMEM((units, quarter), BF),
            pltpu.VMEM((units, quarter), BF),
            pltpu.VMEM((units, quarter), BF),
        ),
        in_specs=[vmem] * 2 + [hbm] * 5,
        out_specs=(vmem,) * 4,
        scratch_shapes=[
            pltpu.VMEM((sides * block, count), BF),
            pltpu.VMEM((sides, count, block), BF),
            pltpu.VMEM((sides * block, 1), F32),
            pltpu.VMEM((rows, rows), BF),
            pltpu.VMEM((rows, rows), BF),
            pltpu.VMEM((2, count, width), BF),
            pltpu.VMEM((2, plane, block, quarter), BF),
            pltpu.VMEM((2, rows, quarter), BF),
            pltpu.VMEM((2, rows, quarter), BF),
            pltpu.VMEM((2, 2 * rows, quarter), BF),
            pltpu.VMEM((4 * units, quarter), BF),
            pltpu.VMEM((2 * units, quarter), BF),
            pltpu.VMEM((2 * rows, 6 * units), F32),
            pltpu.VMEM((2, half, 6 * units), BF),
            pltpu.VMEM((2, half, 6 * units), BF),
            pltpu.VMEM((2, half, 6 * units), BF),
            pltpu.VMEM((2, half, 6 * units), BF),
            pltpu.VMEM((2 * rows, 2 * units), BF),
            pltpu.VMEM((2 * units, 2 * rows), BF),
            pltpu.VMEM((2 * rows, 4 * units), BF),
            pltpu.VMEM((4 * units, 2 * rows), BF),
            pltpu.VMEM((3, units, quarter), BF),
            pltpu.VMEM((3, units, quarter), BF),
            pltpu.VMEM((3, units, quarter), BF),
            pltpu.VMEM((rows, quarter), BF),
            pltpu.VMEM((rows, quarter), BF),
            pltpu.VMEM((rows, quarter), F32),
            pltpu.VMEM((rows, quarter), BF),
            pltpu.VMEM((rows, quarter), BF),
            pltpu.VMEM((rows, quarter), BF),
            pltpu.VMEM((plane, block, quarter), BF),
            pltpu.SemaphoreType.DMA((5,)),
            pltpu.SemaphoreType.DMA((SENDERS,)),
            pltpu.SemaphoreType.DMA((receivers(planes),)),
        ],
        compiler_params=pltpu.CompilerParams(
            collective_id=0, has_side_effects=True, vmem_limit_bytes=58 * 1024 * 1024
        ),
        name="expert_backward",
    )(
        expert_ids.reshape(1, count), route_weight.reshape(1, count),
        tokens, out_grad, w_gate, w_up, w_down,
    )
    return pl.pallas_call(
        store,
        out_shape=tuple(jax.ShapeDtypeStruct(a.shape, a.dtype) for a in results),
        in_specs=[vmem] * 4,
        out_specs=(hbm,) * 4,
        scratch_shapes=[pltpu.SemaphoreType.DMA((4,))],
        compiler_params=pltpu.CompilerParams(vmem_limit_bytes=1024 * 1024),
        name="store",
    )(*(pltpu.with_memory_space_constraint(a, pltpu.VMEM) for a in results))


def solution(mesh):
    tokens = P(("dp", "ep"), None)
    weights = P("dp", "ep")
    planes = mesh.shape["ep"] // PLANE
    return jax.shard_map(
        functools.partial(body, planes, PLANE, CAP),
        mesh=mesh,
        in_specs=(tokens, tokens, tokens, tokens, weights, weights, weights),
        out_specs=(tokens, weights, weights, weights),
        check_vma=False,
    )
```

```python
import functools

import jax
import jax.numpy as jnp
from jax import lax
from jax.experimental import pallas as pl
from jax.experimental.pallas import tpu as pltpu
from jax.sharding import PartitionSpec as P

D = 7168
GROUP = 4
CAP = 6
PLANE = 8
NT = (((1,), (1,)), ((), ()))
NN = (((1,), (0,)), ((), ()))
MESH = pl.DeviceIdType.MESH
BF = jnp.bfloat16
F32 = jnp.float32


def scope(stage):
    @functools.wraps(stage)
    def named(*args):
        tag = "_".join(str(a) for a in args if isinstance(a, int))
        with jax.named_scope(f"{stage.__name__}_{tag}"):
            return stage(*args)

    return named


class Copies:
    def __init__(self, send, recv):
        self.send, self.recv, self.sends, self.recvs, self.open = send, recv, 0, 0, []

    def sender(self, whole):
        self.open.append((whole, self.sends))
        self.sends += 1
        return self.sends - 1

    def slots(self, count):
        self.recvs += count
        return self.recvs - count

    def make(self, src, dst, sent, slot, device):
        return pltpu.make_async_remote_copy(
            src_ref=src,
            dst_ref=dst,
            send_sem=self.send.at[sent],
            recv_sem=self.recv.at[slot],
            device_id=device,
            device_id_type=MESH,
        )

    def start(self, src, dst, sent, slot, device):
        self.make(src, dst, sent, slot, device).start()

    def arrived(self, whole, slot, device):
        self.make(whole, whole, 0, slot, device).wait_recv()

    def drain(self, device):
        for whole, sent in self.open:
            self.make(whole, whole, sent, 0, device).wait_send()


def cut(width, sizes):
    unit, at, out = width // 14, 0, []
    for size in sizes:
        out.append((at, size * unit))
        at += size * unit
    return out


IN_CUTS = ((2, 2, 3, 4, 3), (4, 4, 4, 2))
OUT_CUT = (2, 2, 2, 2, 2, 2, 1, 1)
GRAD_CUT = (4, 4, 4, 2)
SENDERS = 15


def receivers(planes):
    chunks = len(IN_CUTS[0]) + len(IN_CUTS[1])
    return chunks * (2 + planes // 2) - planes // 2 + 1 + 3 * len(OUT_CUT) + 3 + 6 + 6 + 1 + 2 + 3


def slot_tables(planes, plane, cap, ids_ref, rw_ref, sel_ref, sel_t_ref, scale_ref, perm_ref, perm_t_ref):
    count = ids_ref.shape[1]
    block, rows, sides = planes * cap, perm_ref.shape[0], plane // GROUP
    by_col = jnp.broadcast_to(ids_ref[...].astype(F32), (count, count))
    by_row = by_col.T
    i = lax.broadcasted_iota(jnp.int32, (count, count), 0)
    j = lax.broadcasted_iota(jnp.int32, (count, count), 1)
    same = by_col == by_row
    rank_col = jnp.sum(jnp.where(same & (i < j), 1.0, 0.0), axis=0, keepdims=True)
    rank_row = jnp.sum(jnp.where(same & (j < i), 1.0, 0.0), axis=1, keepdims=True)

    def wanted(shape, axis, side_rows):
        at = lax.broadcasted_iota(jnp.int32, shape, axis)
        side, at = at // side_rows, lax.rem(at, side_rows)
        expert = at // cap * sides + side
        return expert.astype(F32), lax.rem(at, cap).astype(F32)

    expert, rank = wanted((sides * block, count), 0, block)
    match = (by_col[:1] == expert) & (rank_col == rank)
    sel_ref[...] = jnp.where(match, 1.0, 0.0).astype(BF)
    scale_ref[...] = jnp.sum(jnp.where(match, rw_ref[...], 0.0), axis=1, keepdims=True)
    expert, rank = wanted((count, block), 1, block)
    for side in range(sides):
        match = (by_row[:, :1] == expert + float(side)) & (rank_row == rank)
        sel_t_ref[side] = jnp.where(match, 1.0, 0.0).astype(BF)

    def source(shape, axis):
        at = lax.broadcasted_iota(jnp.int32, shape, axis)
        zi, rest = at // (plane * cap), lax.rem(at, plane * cap)
        return rest // cap * block + zi * cap + lax.rem(rest, cap)

    i = lax.broadcasted_iota(jnp.int32, (rows, rows), 0)
    j = lax.broadcasted_iota(jnp.int32, (rows, rows), 1)
    perm_ref[...] = jnp.where(source((rows, 1), 0) == j, 1.0, 0.0).astype(BF)
    perm_t_ref[...] = jnp.where(source((1, rows), 1) == i, 1.0, 0.0).astype(BF)


def kernel(
    planes, plane, cap,
    ids_ref, rw_ref, tok_hbm, grad_hbm, wg_hbm, wu_hbm, wd_hbm,
    out_ref, og_ref, ou_ref, od_ref,
    sel_ref, sel_t_ref, scale_ref, perm_ref, perm_t_ref, raw,
    send1, ez, ez_in, er, r1, r1p, xs, wgu, wdn, acc, core_out, core_in, chip_out, chip_in,
    hid, hid_t, dgu, dgu_t, gterm, gown, grecv, dx_send, dx_recv, dx_own, dxs, rz, rzp, ret,
    local_sem, send_sem, recv_sem,
):
    quarter = xs.shape[2]
    block = planes * cap
    rows = plane * block
    half = rows // 2
    units = hid.shape[1] // 2
    r = lax.axis_index("dp")
    ep = lax.axis_index("ep")
    z = ep // plane
    u = lax.rem(ep, plane)
    c = lax.rem(u, 2)
    copies = Copies(send_sem, recv_sem)

    def in_plane(k):
        out = u
        for bit in range(3):
            if k >> bit & 1:
                out = out + (1 << bit) * (1 - 2 * lax.rem(u // (1 << bit), 2))
        return out

    def at_u(k):
        return (r, z * plane + in_plane(k))

    def across(k):
        return (r + 1 - 2 * lax.rem(r, 2), z * plane + in_plane(k))

    def z_to(k):
        return lax.rem(z + k, planes)

    def z_from(k):
        return lax.rem(z + planes - k, planes)

    def at_z(k):
        return (r, z_to(k) * plane + u)

    def from_z(k):
        return (r, z_from(k) * plane + u)

    def blk(index):
        return pl.ds(pl.multiple_of(index * block, block), block)

    def other(index):
        return pl.ds(pl.multiple_of(rows + index * block, block), block)

    reach = [sorted({k, planes - k}) for k in range(1, planes // 2 + 1)]
    z_order = [k for group in reach for k in group]
    u_order = [k for k in (4, 5, 2, 3, 6, 7, 1) if k < plane]
    token_y, weight_y = (r + 1 - 2 * lax.rem(r, 2), ep), (3 - r, ep)

    own_w = (
        (wg_hbm, wgu.at[pl.ds(0, units)], wgu.at[pl.ds(2 * units, units)]),
        (wu_hbm, wgu.at[pl.ds(units, units)], wgu.at[pl.ds(3 * units, units)]),
        (wd_hbm, wdn.at[pl.ds(0, units)], wdn.at[pl.ds(units, units)]),
    )
    lead = quarter // 14 * sum(IN_CUTS[0][:2])
    ahead = [
        pltpu.make_async_copy(
            tok_hbm.at[:, pl.ds(q * quarter + lo, width)],
            raw.at[0, :, pl.ds(q * quarter + lo, width)],
            local_sem.at[n],
        )
        for n, lo, width in ((5, 0, lead), (0, lead, quarter - lead))
        for q in range(GROUP)
    ]
    loads = [
        pltpu.make_async_copy(tok_hbm.at[:, pl.ds(0, GROUP * (quarter - lead))], raw.at[0, :, pl.ds(0, GROUP * (quarter - lead))], local_sem.at[0]),
        pltpu.make_async_copy(grad_hbm, raw.at[1], local_sem.at[1]),
    ]
    for w, (ref, here, _) in enumerate(own_w):
        loads.append(pltpu.make_async_copy(ref, here, local_sem.at[2 + w]))
    for load in ahead:
        load.start()

    barrier = pltpu.get_barrier_semaphore()
    partners = [at_u(k) for k in u_order] + [at_z(k) for k in z_order] + [token_y, weight_y]
    partners += [across(k) for k in u_order]
    for device in partners:
        pl.semaphore_signal(barrier, inc=1, device_id=device, device_id_type=MESH)

    with jax.named_scope("tables"):
        slot_tables(
            planes, plane, cap, ids_ref, rw_ref, sel_ref, sel_t_ref, scale_ref, perm_ref, perm_t_ref
        )
    w_slot = copies.slots(3)
    w_sent = copies.sender(wgu.at[pl.ds(0, 3 * units)])

    @scope
    def weight_here(w):
        loads[2 + w].wait()

    @scope
    def weight(w):
        copies.arrived(own_w[w][2], w_slot + w, weight_y)

    chunks = [cut(quarter, sizes) for sizes in IN_CUTS]
    index = [[0, 1, 2, 3, 4], [5, 6, 7, 8]]
    total = len(IN_CUTS[0]) + len(IN_CUTS[1])
    st1, fwd = copies.slots(total), copies.slots(total)
    early, st2 = copies.slots(1), copies.slots((total - 1) * len(reach)) - len(reach)
    st1_sent = [copies.sender(r1p.at[a, pl.ds(0, rows - block)]) for a in range(2)]
    st2_sent = [copies.sender(r1p.at[a, pl.ds(0, rows - rows // planes)]) for a in range(2)]
    fwd_sent = [copies.sender(xs.at[a, pl.ds(0, rows)]) for a in range(2)]

    @scope
    def gather(a, j):
        lo, width = chunks[a][j]
        cols = pl.ds(lo, width)
        for q in range(GROUP):
            got = lax.dot_general(
                sel_ref[...], raw[a, :, pl.ds(q * quarter + lo, width)], NN, preferred_element_type=F32
            )
            if a:
                got = got * scale_ref[...]
            got = got.astype(BF)
            for h in range(plane // GROUP):
                send1[a, pl.ds((h * GROUP + q) * block, block), cols] = got[h * block : (h + 1) * block]

    @scope
    def to_plane(a, j):
        cols = pl.ds(*chunks[a][j])
        r1[a, blk(u), cols] = send1[a, blk(u), cols]
        for k in u_order:
            copies.start(
                send1.at[a, blk(in_plane(k)), cols],
                r1.at[a, blk(u), cols],
                st1_sent[a],
                st1 + index[a][j],
                at_u(k),
            )

    @scope
    def plane_stage(a, j):
        cols = pl.ds(*chunks[a][j])
        copies.arrived(r1.at[a, pl.ds(0, rows - block), cols], st1 + index[a][j], at_u(1))
        r1p[a, :, cols] = lax.dot_general(
            perm_ref[...], r1[a, :, cols], NN, preferred_element_type=F32
        ).astype(BF)
        for g, group in enumerate(reach):
            for k in group:
                copies.start(
                    r1p.at[a, blk(z_to(k)), cols],
                    xs.at[a, blk(z), cols],
                    st2_sent[a],
                    st2 + index[a][j] * len(reach) + g,
                    at_z(k),
                )
        xs[a, blk(z), cols] = r1p[a, blk(z), cols]
        pass_on(a, j, 0)

    first = pl.ds(*chunks[0][0])

    @scope
    def early_z():
        ez[...] = lax.dot_general(
            perm_ref[...], send1[0, :, first], NN, preferred_element_type=F32
        ).astype(BF)
        for k in z_order:
            copies.start(ez.at[blk(z_to(k))], ez_in.at[blk(z)], st2_sent[0], early, at_z(k))
        ez_in[blk(z)] = ez[blk(z)]

    @scope
    def early_plane():
        copies.arrived(ez_in.at[pl.ds(0, rows - rows // planes)], early, at_z(1))
        r1p[0, :, first] = lax.dot_general(
            perm_t_ref[...], ez_in[...], NN, preferred_element_type=F32
        ).astype(BF)
        for k in u_order:
            copies.start(
                r1p.at[0, blk(in_plane(k)), first], r1.at[0, blk(u), first], st1_sent[0], st1, at_u(k)
            )
        for k in [0] + u_order:
            copies.start(
                r1p.at[0, blk(in_plane(k)), first], er.at[blk(u)], fwd_sent[0], fwd, across(k)
            )
        r1[0, blk(u), first] = r1p[0, blk(u), first]

    @scope
    def early_here(t):
        if t:
            copies.arrived(er, fwd, token_y)
        else:
            copies.arrived(r1.at[0, pl.ds(0, rows - block), first], st1, at_u(1))
        src = er[...] if t else r1[0, :, first]
        xs[0, pl.ds(t * rows, rows), first] = lax.dot_general(
            perm_ref[...], src, NN, preferred_element_type=F32
        ).astype(BF)

    @scope
    def forward(a, j, g0, g1):
        cols = pl.ds(*chunks[a][j])
        for g in range(g0, min(g1, len(reach))):
            copies.arrived(
                xs.at[a, pl.ds(0, len(reach[g]) * block), cols],
                st2 + index[a][j] * len(reach) + g,
                at_z(1),
            )
            for k in reach[g]:
                pass_on(a, j, k)

    def pass_on(a, j, k):
        cols = pl.ds(*chunks[a][j])
        zs = z_from(k)
        copies.start(
            xs.at[a, blk(zs), cols], xs.at[a, other(zs), cols], fwd_sent[a], fwd + index[a][j], token_y
        )

    @scope
    def forwarded(a, j):
        cols = pl.ds(*chunks[a][j])
        copies.arrived(xs.at[a, pl.ds(rows, rows), cols], fwd + index[a][j], token_y)

    mine = lambda t: pl.ds(pl.multiple_of(t * rows + c * half, half), half)
    theirs = lambda t: pl.ds(pl.multiple_of(t * rows + (1 - c) * half, half), half)
    core = copies.slots(6)
    chip = copies.slots(6)
    share_h, share_d = copies.slots(1), copies.slots(2)
    core_sent, chip_sent = copies.sender(core_out), copies.sender(chip_out)
    h_sent, d_sent = copies.sender(hid.at[pl.ds(0, rows)]), copies.sender(dgu.at[pl.ds(0, rows)])
    span = 2 * units

    def project(left, weights, t, g, cols, add):
        at = pl.ds(t * rows, rows)

        def step(b, carry):
            got = lax.dot_general(
                left[at, cols],
                weights[pl.ds(pl.multiple_of(b * units, units), units), cols],
                NT,
                preferred_element_type=F32,
            )
            to = pl.ds(pl.multiple_of(g * span + b * units, units), units)
            acc[at, to] = acc[at, to] + got if add else got
            return carry

        lax.fori_loop(0, 2, step, 0)

    @scope
    def gate_up(t, b):
        project(xs.at[0], wgu.at[pl.ds(b * span, span)], t, b, pl.ds(0, quarter), False)

    @scope
    def back(t, j0, j1):
        lo = chunks[1][j0][0]
        width = sum(chunks[1][j1]) - lo
        project(xs.at[1], wdn, t, 2, pl.ds(lo, width), j0 > 0)

    @scope
    def to_core(t, g):
        cols = pl.ds(g * span, span)
        core_out[t, :, cols] = acc[theirs(t), cols].astype(BF)
        copies.start(core_out.at[t, :, cols], core_in.at[t, :, cols], core_sent, core + 3 * t + g, at_u(1))

    @scope
    def to_chip(t, g):
        cols = pl.ds(g * span, span)
        copies.arrived(core_in.at[t, :, cols], core + 3 * t + g, at_u(1))
        pair = acc[mine(t), cols] + core_in[t, :, cols].astype(F32)
        acc[mine(t), cols] = pair
        chip_out[t, :, cols] = pair.astype(BF)
        copies.start(chip_out.at[t, :, cols], chip_in.at[t, :, cols], chip_sent, chip + 3 * t + g, at_u(2))

    def summed(t, g):
        cols = pl.ds(g * span, span)
        copies.arrived(chip_in.at[t, :, cols], chip + 3 * t + g, at_u(2))
        return acc[mine(t), cols] + chip_in[t, :, cols].astype(F32)

    @scope
    def hidden(t, b):
        both = summed(t, b)
        acc[mine(t), pl.ds(b * span, span)] = both
        gate, up = both[:, :units], both[:, units:]
        at = hid.at[mine(t), pl.ds(b * units, units)]
        at[...] = (gate * jax.nn.sigmoid(gate) * up).astype(BF)
        copies.start(at, at, h_sent, share_h, at_u(1))

    @scope
    def gradients(t):
        both = summed(t, 2)
        for b in range(2):
            gate = acc[mine(t), pl.ds(b * span, units)]
            up = acc[mine(t), pl.ds(b * span + units, units)]
            grad = both[:, b * units : (b + 1) * units]
            logistic = jax.nn.sigmoid(gate)
            dgu[mine(t), pl.ds(b * span, units)] = (
                grad * up * logistic * (1.0 + gate * (1.0 - logistic))
            ).astype(BF)
            dgu[mine(t), pl.ds(b * span + units, units)] = (grad * (gate * logistic)).astype(BF)
        at = dgu.at[mine(t)]
        copies.start(at, at, d_sent, share_d + t, at_u(1))

    @scope
    def hidden_here():
        copies.arrived(hid.at[pl.ds(0, rows)], share_h, at_u(1))

    @scope
    def gradients_here(t):
        copies.arrived(dgu.at[theirs(t)], share_d + t, at_u(1))

    grad_cut = cut(quarter, GRAD_CUT)
    gr = copies.slots(3)
    gr_sent = copies.sender(gterm)

    @scope
    def flip_hidden():
        hid_t[...] = hid[...].T

    @scope
    def flip_gradients(b):
        dgu_t[pl.ds(b * span, span)] = dgu[:, pl.ds(b * span, span)].T

    @scope
    def down_out(i):
        cols = pl.ds(*grad_cut[i])
        gterm[2, :, cols] = lax.dot_general(
            hid_t[pl.ds(units, units)], xs[1, :, cols], NN, preferred_element_type=F32
        ).astype(BF)
        copies.start(gterm.at[2, :, cols], grecv.at[2, :, cols], gr_sent, gr + 2, weight_y)

    @scope
    def gate_up_out(i):
        cols = pl.ds(*grad_cut[i])
        for w in range(2):
            gterm[w, :, cols] = lax.dot_general(
                dgu_t[pl.ds(span + w * units, units)], xs[0, :, cols], NN, preferred_element_type=F32
            ).astype(BF)
            copies.start(gterm.at[w, :, cols], grecv.at[w, :, cols], gr_sent, gr + w, weight_y)

    @scope
    def term_here(w):
        left = hid_t.at[pl.ds(0, units)] if w == 2 else dgu_t.at[pl.ds(w * units, units)]
        for lo, width in grad_cut:
            cols = pl.ds(lo, width)
            gown[w, :, cols] = lax.dot_general(
                left[...], xs[w // 2, :, cols], NN, preferred_element_type=F32
            ).astype(BF)

    @scope
    def grad_out(w, ref):
        copies.arrived(grecv.at[w], gr + w, weight_y)
        ref[...] = (gown[w].astype(F32) + grecv[w].astype(F32)).astype(BF)

    parts = cut(quarter, OUT_CUT)
    dxy = copies.slots(len(parts))
    dxz, dxu = copies.slots(len(parts)), copies.slots(len(parts))
    dxy_sent = copies.sender(dx_send)
    dxz_sent = copies.sender(dxs.at[pl.ds(0, rows - rows // planes)])
    dxu_sent = copies.sender(dxs.at[pl.ds(0, rows - block)])

    def dx_term(t, cols):
        return lax.dot_general(
            dgu[pl.ds(t * rows, rows)], wgu[:, cols], NN, preferred_element_type=F32
        )

    @scope
    def dx_out(i):
        cols = pl.ds(*parts[i])
        dx_send[:, cols] = dx_term(1, cols).astype(BF)
        copies.start(dx_send.at[:, cols], dx_recv.at[:, cols], dxy_sent, dxy + i, token_y)

    @scope
    def dx_here(i):
        cols = pl.ds(*parts[i])
        dx_own[:, cols] = dx_term(0, cols)

    @scope
    def dx_z(i):
        cols = pl.ds(*parts[i])
        copies.arrived(dx_recv.at[:, cols], dxy + i, token_y)
        dxs[:, cols] = (dx_own[:, cols] + dx_recv[:, cols].astype(F32)).astype(BF)
        for k in reversed(z_order):
            copies.start(
                dxs.at[blk(z_to(k)), cols], rz.at[blk(z), cols], dxz_sent, dxz + i, at_z(k)
            )
        rz[blk(z), cols] = dxs[blk(z), cols]

    @scope
    def dx_u(i):
        cols = pl.ds(*parts[i])
        copies.arrived(rz.at[pl.ds(0, rows - rows // planes), cols], dxz + i, at_z(1))
        rzp[:, cols] = lax.dot_general(
            perm_t_ref[...], rz[:, cols], NN, preferred_element_type=F32
        ).astype(BF)
        for k in u_order:
            copies.start(
                rzp.at[blk(in_plane(k)), cols], ret.at[u, :, cols], dxu_sent, dxu + i, at_u(k)
            )
        ret[u, :, cols] = rzp[blk(u), cols]

    @scope
    def dx_back(i):
        lo, width = parts[i]
        cols = pl.ds(lo, width)
        copies.arrived(rz.at[pl.ds(0, rows - block), cols], dxu + i, at_u(1))
        for q in range(GROUP):
            total = None
            for h in range(plane // GROUP):
                got = lax.dot_general(
                    sel_t_ref[h], ret[h * GROUP + q, :, cols], NN, preferred_element_type=F32
                )
                total = got if total is None else total + got
            out_ref[:, pl.ds(q * quarter + lo, width)] = total.astype(BF)

    pltpu.make_async_copy(
        tok_hbm.at[:, pl.ds(0, GROUP * lead)], raw.at[0, :, pl.ds(0, GROUP * lead)], local_sem.at[5]
    ).wait()
    for load in loads[1:]:
        load.start()
    gather(0, 0)
    gather(0, 1)
    with jax.named_scope("barrier"):
        pl.semaphore_wait(barrier, len(partners))
    to_plane(0, 1)
    early_z()
    for w, (ref, _, there) in enumerate(own_w):
        copies.start(ref, there, w_sent, w_slot + w, weight_y)
    loads[0].wait()
    for j in range(2, 5):
        gather(0, j)
        to_plane(0, j)
    loads[1].wait()
    gather(1, 0)
    gather(1, 1)
    plane_stage(0, 1)
    early_plane()
    plane_stage(0, 2)
    to_plane(1, 0)
    to_plane(1, 1)
    gather(1, 2)
    to_plane(1, 2)
    gather(1, 3)
    to_plane(1, 3)
    forward(0, 1, 0, 4)
    plane_stage(0, 3)
    forward(0, 2, 0, 2)
    early_here(0)
    forward(0, 2, 2, 4)
    plane_stage(0, 4)
    forward(0, 3, 0, 1)
    early_here(1)
    forward(0, 3, 1, 4)
    plane_stage(1, 0)
    forward(0, 4, 0, 4)
    plane_stage(1, 1)
    weight_here(0)
    weight_here(1)
    gate_up(0, 0)
    to_core(0, 0)
    forward(1, 0, 0, 1)
    for j in range(1, 5):
        forwarded(0, j)
    gate_up(1, 0)
    to_core(1, 0)
    to_chip(0, 0)
    forward(1, 0, 1, 2)
    weight(0)
    weight(1)
    gate_up(0, 1)
    to_core(0, 1)
    to_chip(1, 0)
    gate_up(1, 1)
    to_core(1, 1)
    forward(1, 0, 2, 4)
    to_chip(0, 1)
    plane_stage(1, 2)
    to_chip(1, 1)
    plane_stage(1, 3)
    forward(1, 1, 0, 1)
    hidden(0, 0)
    forward(1, 1, 1, 4)
    hidden(1, 0)
    forward(1, 2, 0, 2)
    hidden(0, 1)
    forward(1, 2, 2, 3)
    hidden(1, 1)
    forward(1, 2, 3, 4)
    hidden_here()
    flip_hidden()
    forwarded(1, 0)
    down_out(0)
    forward(1, 3, 0, 1)
    forwarded(1, 1)
    down_out(1)
    weight_here(2)
    weight(2)
    forward(1, 3, 1, 2)
    back(0, 0, 2)
    forward(1, 3, 2, 3)
    back(1, 0, 1)
    forward(1, 3, 3, 4)
    back(0, 3, 3)
    to_core(0, 2)
    forwarded(1, 2)
    back(1, 2, 2)
    to_chip(0, 2)
    forwarded(1, 3)
    back(1, 3, 3)
    to_core(1, 2)
    down_out(2)
    to_chip(1, 2)
    gradients(0)
    down_out(3)
    gradients(1)
    gradients_here(0)
    gradients_here(1)
    dx_out(0)
    flip_gradients(1)
    gate_up_out(0)
    dx_out(1)
    gate_up_out(1)
    dx_out(2)
    dx_here(0)
    dx_out(3)
    gate_up_out(2)
    dx_z(0)
    dx_out(4)
    gate_up_out(3)
    dx_out(5)
    dx_here(1)
    dx_z(1)
    dx_out(6)
    dx_out(7)
    dx_here(2)
    dx_here(3)
    dx_z(2)
    dx_u(0)
    dx_here(4)
    dx_here(5)
    dx_z(3)
    dx_u(1)
    dx_here(6)
    dx_here(7)
    flip_gradients(0)
    dx_z(4)
    dx_u(2)
    dx_back(0)
    term_here(2)
    dx_z(5)
    dx_u(3)
    dx_back(1)
    term_here(0)
    dx_z(6)
    dx_u(4)
    dx_back(2)
    dx_z(7)
    term_here(1)
    dx_u(5)
    dx_back(3)
    dx_u(6)
    dx_back(4)
    dx_u(7)
    grad_out(2, od_ref)
    dx_back(5)
    dx_back(6)
    dx_back(7)
    grad_out(0, og_ref)
    grad_out(1, ou_ref)
    with jax.named_scope("drain"):
        copies.drain(token_y)
    assert (copies.sends, copies.recvs) == (SENDERS, receivers(planes))


def store(*refs):
    sems = refs[-1]
    moves = [pltpu.make_async_copy(refs[i], refs[4 + i], sems.at[i]) for i in range(4)]
    for move in moves:
        move.start()
    for move in moves:
        move.wait()


def body(planes, plane, capacity, tokens, out_grad, route_weight, expert_ids, w_gate, w_up, w_down):
    count, width = tokens.shape
    quarter = width // GROUP
    units = w_gate.shape[0]
    block = planes * capacity
    rows = plane * block
    half = rows // 2
    sides = plane // GROUP
    vmem = pl.BlockSpec(memory_space=pltpu.VMEM)
    hbm = pl.BlockSpec(memory_space=pl.ANY)
    results = pl.pallas_call(
        functools.partial(kernel, planes, plane, capacity),
        out_shape=(
            pltpu.VMEM((count, width), BF),
            pltpu.VMEM((units, quarter), BF),
            pltpu.VMEM((units, quarter), BF),
            pltpu.VMEM((units, quarter), BF),
        ),
        in_specs=[vmem] * 2 + [hbm] * 5,
        out_specs=(vmem,) * 4,
        scratch_shapes=[
            pltpu.VMEM((sides * block, count), BF),
            pltpu.VMEM((sides, count, block), BF),
            pltpu.VMEM((sides * block, 1), F32),
            pltpu.VMEM((rows, rows), BF),
            pltpu.VMEM((rows, rows), BF),
            pltpu.VMEM((2, count, width), BF),
            pltpu.VMEM((2, rows, quarter), BF),
            pltpu.VMEM((rows, quarter // 14 * IN_CUTS[0][0]), BF),
            pltpu.VMEM((rows, quarter // 14 * IN_CUTS[0][0]), BF),
            pltpu.VMEM((rows, quarter // 14 * IN_CUTS[0][0]), BF),
            pltpu.VMEM((2, rows, quarter), BF),
            pltpu.VMEM((2, rows, quarter), BF),
            pltpu.VMEM((2, 2 * rows, quarter), BF),
            pltpu.VMEM((4 * units, quarter), BF),
            pltpu.VMEM((2 * units, quarter), BF),
            pltpu.VMEM((2 * rows, 6 * units), F32),
            pltpu.VMEM((2, half, 6 * units), BF),
            pltpu.VMEM((2, half, 6 * units), BF),
            pltpu.VMEM((2, half, 6 * units), BF),
            pltpu.VMEM((2, half, 6 * units), BF),
            pltpu.VMEM((2 * rows, 2 * units), BF),
            pltpu.VMEM((2 * units, 2 * rows), BF),
            pltpu.VMEM((2 * rows, 4 * units), BF),
            pltpu.VMEM((4 * units, 2 * rows), BF),
            pltpu.VMEM((3, units, quarter), BF),
            pltpu.VMEM((3, units, quarter), BF),
            pltpu.VMEM((3, units, quarter), BF),
            pltpu.VMEM((rows, quarter), BF),
            pltpu.VMEM((rows, quarter), BF),
            pltpu.VMEM((rows, quarter), F32),
            pltpu.VMEM((rows, quarter), BF),
            pltpu.VMEM((rows, quarter), BF),
            pltpu.VMEM((rows, quarter), BF),
            pltpu.VMEM((plane, block, quarter), BF),
            pltpu.SemaphoreType.DMA((6,)),
            pltpu.SemaphoreType.DMA((SENDERS,)),
            pltpu.SemaphoreType.DMA((receivers(planes),)),
        ],
        compiler_params=pltpu.CompilerParams(
            collective_id=0, has_side_effects=True, vmem_limit_bytes=58 * 1024 * 1024
        ),
        name="expert_backward",
    )(
        expert_ids.reshape(1, count), route_weight.reshape(1, count),
        tokens, out_grad, w_gate, w_up, w_down,
    )
    return pl.pallas_call(
        store,
        out_shape=tuple(jax.ShapeDtypeStruct(a.shape, a.dtype) for a in results),
        in_specs=[vmem] * 4,
        out_specs=(hbm,) * 4,
        scratch_shapes=[pltpu.SemaphoreType.DMA((4,))],
        compiler_params=pltpu.CompilerParams(vmem_limit_bytes=1024 * 1024),
        name="store",
    )(*(pltpu.with_memory_space_constraint(a, pltpu.VMEM) for a in results))


def solution(mesh):
    tokens = P(("dp", "ep"), None)
    weights = P("dp", "ep")
    planes = mesh.shape["ep"] // PLANE
    return jax.shard_map(
        functools.partial(body, planes, PLANE, CAP),
        mesh=mesh,
        in_specs=(tokens, tokens, tokens, tokens, weights, weights, weights),
        out_specs=(tokens, weights, weights, weights),
        check_vma=False,
    )
```

```python
import functools

import jax
import jax.numpy as jnp
from jax import lax
from jax.experimental import pallas as pl
from jax.experimental.pallas import tpu as pltpu
from jax.sharding import PartitionSpec as P

D = 7168
GROUP = 4
CAP = 6
PLANE = 8
NT = (((1,), (1,)), ((), ()))
NN = (((1,), (0,)), ((), ()))
MESH = pl.DeviceIdType.MESH
BF = jnp.bfloat16
F32 = jnp.float32


def scope(stage):
    @functools.wraps(stage)
    def named(*args):
        tag = "_".join(str(a) for a in args if isinstance(a, int))
        with jax.named_scope(f"{stage.__name__}_{tag}"):
            return stage(*args)

    return named


class Copies:
    def __init__(self, send, recv):
        self.send, self.recv, self.sends, self.recvs, self.open = send, recv, 0, 0, []

    def sender(self, whole):
        self.open.append((whole, self.sends))
        self.sends += 1
        return self.sends - 1

    def slots(self, count):
        self.recvs += count
        return self.recvs - count

    def make(self, src, dst, sent, slot, device):
        return pltpu.make_async_remote_copy(
            src_ref=src,
            dst_ref=dst,
            send_sem=self.send.at[sent],
            recv_sem=self.recv.at[slot],
            device_id=device,
            device_id_type=MESH,
        )

    def start(self, src, dst, sent, slot, device):
        self.make(src, dst, sent, slot, device).start()

    def arrived(self, whole, slot, device):
        self.make(whole, whole, 0, slot, device).wait_recv()

    def drain(self, device):
        for whole, sent in self.open:
            self.make(whole, whole, sent, 0, device).wait_send()


def cut(width, sizes):
    unit, at, out = width // 14, 0, []
    for size in sizes:
        out.append((at, size * unit))
        at += size * unit
    return out


IN_CUTS = ((2, 2, 3, 4, 3), (4, 4, 4, 2))
OUT_CUT = (2, 2, 2, 2, 2, 2, 1, 1)
GRAD_CUT = (4, 4, 4, 2)
SENDERS = 15


def receivers(planes):
    chunks = len(IN_CUTS[0]) + len(IN_CUTS[1])
    return chunks * (2 + planes // 2) - planes // 2 + 1 + 3 * len(OUT_CUT) + 3 + 6 + 6 + 1 + 2 + 3


def slot_tables(planes, plane, cap, ids_ref, rw_ref, sel_ref, sel_t_ref, scale_ref, perm_ref, perm_t_ref):
    count = ids_ref.shape[1]
    block, rows, sides = planes * cap, perm_ref.shape[0], plane // GROUP
    by_col = jnp.broadcast_to(ids_ref[...].astype(F32), (count, count))
    by_row = by_col.T
    i = lax.broadcasted_iota(jnp.int32, (count, count), 0)
    j = lax.broadcasted_iota(jnp.int32, (count, count), 1)
    same = by_col == by_row
    rank_col = jnp.sum(jnp.where(same & (i < j), 1.0, 0.0), axis=0, keepdims=True)
    rank_row = jnp.sum(jnp.where(same & (j < i), 1.0, 0.0), axis=1, keepdims=True)

    def wanted(shape, axis, side_rows):
        at = lax.broadcasted_iota(jnp.int32, shape, axis)
        side, at = at // side_rows, lax.rem(at, side_rows)
        expert = at // cap * sides + side
        return expert.astype(F32), lax.rem(at, cap).astype(F32)

    expert, rank = wanted((sides * block, count), 0, block)
    match = (by_col[:1] == expert) & (rank_col == rank)
    sel_ref[...] = jnp.where(match, 1.0, 0.0).astype(BF)
    scale_ref[...] = jnp.sum(jnp.where(match, rw_ref[...], 0.0), axis=1, keepdims=True)
    expert, rank = wanted((count, block), 1, block)
    for side in range(sides):
        match = (by_row[:, :1] == expert + float(side)) & (rank_row == rank)
        sel_t_ref[side] = jnp.where(match, 1.0, 0.0).astype(BF)

    def source(shape, axis):
        at = lax.broadcasted_iota(jnp.int32, shape, axis)
        zi, rest = at // (plane * cap), lax.rem(at, plane * cap)
        return rest // cap * block + zi * cap + lax.rem(rest, cap)

    i = lax.broadcasted_iota(jnp.int32, (rows, rows), 0)
    j = lax.broadcasted_iota(jnp.int32, (rows, rows), 1)
    perm_ref[...] = jnp.where(source((rows, 1), 0) == j, 1.0, 0.0).astype(BF)
    perm_t_ref[...] = jnp.where(source((1, rows), 1) == i, 1.0, 0.0).astype(BF)


def kernel(
    planes, plane, cap,
    ids_ref, rw_ref, tok_hbm, grad_hbm, wg_hbm, wu_hbm, wd_hbm,
    out_ref, og_ref, ou_ref, od_ref,
    sel_ref, sel_t_ref, scale_ref, perm_ref, perm_t_ref, raw,
    send1, ez, ez_in, er, r1, r1p, xs, wgu, wdn, acc, core_out, core_in, chip_out, chip_in,
    hid, hid_t, dgu, dgu_t, gterm, gown, grecv, dx_send, dx_recv, dx_own, dxs, rz, rzp, ret,
    local_sem, send_sem, recv_sem,
):
    quarter = xs.shape[2]
    block = planes * cap
    rows = plane * block
    half = rows // 2
    units = hid.shape[1] // 2
    r = lax.axis_index("dp")
    ep = lax.axis_index("ep")
    z = ep // plane
    u = lax.rem(ep, plane)
    c = lax.rem(u, 2)
    copies = Copies(send_sem, recv_sem)

    def in_plane(k):
        out = u
        for bit in range(3):
            if k >> bit & 1:
                out = out + (1 << bit) * (1 - 2 * lax.rem(u // (1 << bit), 2))
        return out

    def at_u(k):
        return (r, z * plane + in_plane(k))

    def across(k):
        return (r + 1 - 2 * lax.rem(r, 2), z * plane + in_plane(k))

    def z_to(k):
        return lax.rem(z + k, planes)

    def z_from(k):
        return lax.rem(z + planes - k, planes)

    def at_z(k):
        return (r, z_to(k) * plane + u)

    def from_z(k):
        return (r, z_from(k) * plane + u)

    def blk(index):
        return pl.ds(pl.multiple_of(index * block, block), block)

    def other(index):
        return pl.ds(pl.multiple_of(rows + index * block, block), block)

    reach = [sorted({k, planes - k}) for k in range(1, planes // 2 + 1)]
    z_order = [k for group in reach for k in group]
    u_order = [k for k in (4, 5, 2, 3, 6, 7, 1) if k < plane]
    token_y, weight_y = (r + 1 - 2 * lax.rem(r, 2), ep), (3 - r, ep)

    own_w = (
        (wg_hbm, wgu.at[pl.ds(0, units)], wgu.at[pl.ds(2 * units, units)]),
        (wu_hbm, wgu.at[pl.ds(units, units)], wgu.at[pl.ds(3 * units, units)]),
        (wd_hbm, wdn.at[pl.ds(0, units)], wdn.at[pl.ds(units, units)]),
    )
    lead = quarter // 14 * sum(IN_CUTS[0][:2])
    ahead = [
        pltpu.make_async_copy(
            tok_hbm.at[:, pl.ds(q * quarter + lo, width)],
            raw.at[0, :, pl.ds(q * quarter + lo, width)],
            local_sem.at[n],
        )
        for n, lo, width in ((5, 0, lead), (0, lead, quarter - lead))
        for q in range(GROUP)
    ]
    loads = [
        pltpu.make_async_copy(tok_hbm.at[:, pl.ds(0, GROUP * (quarter - lead))], raw.at[0, :, pl.ds(0, GROUP * (quarter - lead))], local_sem.at[0]),
        pltpu.make_async_copy(grad_hbm, raw.at[1], local_sem.at[1]),
    ]
    for w, (ref, here, _) in enumerate(own_w):
        loads.append(pltpu.make_async_copy(ref, here, local_sem.at[2 + w]))
    for load in ahead:
        load.start()

    barrier = pltpu.get_barrier_semaphore()
    partners = [at_u(k) for k in u_order] + [at_z(k) for k in z_order] + [token_y, weight_y]
    partners += [across(k) for k in u_order]
    for device in partners:
        pl.semaphore_signal(barrier, inc=1, device_id=device, device_id_type=MESH)

    with jax.named_scope("tables"):
        slot_tables(
            planes, plane, cap, ids_ref, rw_ref, sel_ref, sel_t_ref, scale_ref, perm_ref, perm_t_ref
        )
    w_slot = copies.slots(3)
    w_sent = copies.sender(wgu.at[pl.ds(0, 3 * units)])

    @scope
    def weight_here(w):
        loads[2 + w].wait()

    @scope
    def weight(w):
        copies.arrived(own_w[w][2], w_slot + w, weight_y)

    chunks = [cut(quarter, sizes) for sizes in IN_CUTS]
    index = [[0, 1, 2, 3, 4], [5, 6, 7, 8]]
    total = len(IN_CUTS[0]) + len(IN_CUTS[1])
    st1, fwd = copies.slots(total), copies.slots(total)
    early, st2 = copies.slots(1), copies.slots((total - 1) * len(reach)) - len(reach)
    st1_sent = [copies.sender(r1p.at[a, pl.ds(0, rows - block)]) for a in range(2)]
    st2_sent = [copies.sender(r1p.at[a, pl.ds(0, rows - rows // planes)]) for a in range(2)]
    fwd_sent = [copies.sender(xs.at[a, pl.ds(0, rows)]) for a in range(2)]

    @scope
    def gather(a, j):
        lo, width = chunks[a][j]
        cols = pl.ds(lo, width)
        for q in range(GROUP):
            got = lax.dot_general(
                sel_ref[...], raw[a, :, pl.ds(q * quarter + lo, width)], NN, preferred_element_type=F32
            )
            if a:
                got = got * scale_ref[...]
            got = got.astype(BF)
            for h in range(plane // GROUP):
                send1[a, pl.ds((h * GROUP + q) * block, block), cols] = got[h * block : (h + 1) * block]

    @scope
    def to_plane(a, j):
        cols = pl.ds(*chunks[a][j])
        r1[a, blk(u), cols] = send1[a, blk(u), cols]
        for k in u_order:
            copies.start(
                send1.at[a, blk(in_plane(k)), cols],
                r1.at[a, blk(u), cols],
                st1_sent[a],
                st1 + index[a][j],
                at_u(k),
            )

    @scope
    def plane_stage(a, j):
        cols = pl.ds(*chunks[a][j])
        copies.arrived(r1.at[a, pl.ds(0, rows - block), cols], st1 + index[a][j], at_u(1))
        r1p[a, :, cols] = lax.dot_general(
            perm_ref[...], r1[a, :, cols], NN, preferred_element_type=F32
        ).astype(BF)
        for g, group in enumerate(reach):
            for k in group:
                copies.start(
                    r1p.at[a, blk(z_to(k)), cols],
                    xs.at[a, blk(z), cols],
                    st2_sent[a],
                    st2 + index[a][j] * len(reach) + g,
                    at_z(k),
                )
        xs[a, blk(z), cols] = r1p[a, blk(z), cols]
        pass_on(a, j, 0)

    first = pl.ds(*chunks[0][0])

    @scope
    def early_z():
        ez[...] = lax.dot_general(
            perm_ref[...], send1[0, :, first], NN, preferred_element_type=F32
        ).astype(BF)
        for k in z_order:
            copies.start(ez.at[blk(z_to(k))], ez_in.at[blk(z)], st2_sent[0], early, at_z(k))
        ez_in[blk(z)] = ez[blk(z)]

    @scope
    def early_plane():
        copies.arrived(ez_in.at[pl.ds(0, rows - rows // planes)], early, at_z(1))
        r1p[0, :, first] = lax.dot_general(
            perm_t_ref[...], ez_in[...], NN, preferred_element_type=F32
        ).astype(BF)
        for k in u_order:
            copies.start(
                r1p.at[0, blk(in_plane(k)), first], r1.at[0, blk(u), first], st1_sent[0], st1, at_u(k)
            )
        for k in [0] + u_order:
            copies.start(
                r1p.at[0, blk(in_plane(k)), first], er.at[blk(u)], fwd_sent[0], fwd, across(k)
            )
        r1[0, blk(u), first] = r1p[0, blk(u), first]

    @scope
    def early_here(t):
        if t:
            copies.arrived(er, fwd, token_y)
        else:
            copies.arrived(r1.at[0, pl.ds(0, rows - block), first], st1, at_u(1))
        src = er[...] if t else r1[0, :, first]
        xs[0, pl.ds(t * rows, rows), first] = lax.dot_general(
            perm_ref[...], src, NN, preferred_element_type=F32
        ).astype(BF)

    @scope
    def forward(a, j, g0, g1):
        cols = pl.ds(*chunks[a][j])
        for g in range(g0, min(g1, len(reach))):
            copies.arrived(
                xs.at[a, pl.ds(0, len(reach[g]) * block), cols],
                st2 + index[a][j] * len(reach) + g,
                at_z(1),
            )
            for k in reach[g]:
                pass_on(a, j, k)

    def pass_on(a, j, k):
        cols = pl.ds(*chunks[a][j])
        zs = z_from(k)
        copies.start(
            xs.at[a, blk(zs), cols], xs.at[a, other(zs), cols], fwd_sent[a], fwd + index[a][j], token_y
        )

    @scope
    def forwarded(a, j):
        cols = pl.ds(*chunks[a][j])
        copies.arrived(xs.at[a, pl.ds(rows, rows), cols], fwd + index[a][j], token_y)

    mine = lambda t: pl.ds(pl.multiple_of(t * rows + c * half, half), half)
    theirs = lambda t: pl.ds(pl.multiple_of(t * rows + (1 - c) * half, half), half)
    core = copies.slots(6)
    chip = copies.slots(6)
    share_h, share_d = copies.slots(1), copies.slots(2)
    core_sent, chip_sent = copies.sender(core_out), copies.sender(chip_out)
    h_sent, d_sent = copies.sender(hid.at[pl.ds(0, rows)]), copies.sender(dgu.at[pl.ds(0, rows)])
    span = 2 * units

    def project(left, weights, t, g, cols, add):
        at = pl.ds(t * rows, rows)

        def step(b, carry):
            got = lax.dot_general(
                left[at, cols],
                weights[pl.ds(pl.multiple_of(b * units, units), units), cols],
                NT,
                preferred_element_type=F32,
            )
            to = pl.ds(pl.multiple_of(g * span + b * units, units), units)
            acc[at, to] = acc[at, to] + got if add else got
            return carry

        lax.fori_loop(0, 2, step, 0)

    @scope
    def gate_up(t, b):
        project(xs.at[0], wgu.at[pl.ds(b * span, span)], t, b, pl.ds(0, quarter), False)

    @scope
    def back(t, j0, j1):
        lo = chunks[1][j0][0]
        width = sum(chunks[1][j1]) - lo
        project(xs.at[1], wdn, t, 2, pl.ds(lo, width), j0 > 0)

    @scope
    def to_core(t, g):
        cols = pl.ds(g * span, span)
        core_out[t, :, cols] = acc[theirs(t), cols].astype(BF)
        copies.start(core_out.at[t, :, cols], core_in.at[t, :, cols], core_sent, core + 3 * t + g, at_u(1))

    @scope
    def to_chip(t, g):
        cols = pl.ds(g * span, span)
        copies.arrived(core_in.at[t, :, cols], core + 3 * t + g, at_u(1))
        pair = acc[mine(t), cols] + core_in[t, :, cols].astype(F32)
        acc[mine(t), cols] = pair
        chip_out[t, :, cols] = pair.astype(BF)
        copies.start(chip_out.at[t, :, cols], chip_in.at[t, :, cols], chip_sent, chip + 3 * t + g, at_u(2))

    def summed(t, g):
        cols = pl.ds(g * span, span)
        copies.arrived(chip_in.at[t, :, cols], chip + 3 * t + g, at_u(2))
        return acc[mine(t), cols] + chip_in[t, :, cols].astype(F32)

    @scope
    def hidden(t, b):
        both = summed(t, b)
        acc[mine(t), pl.ds(b * span, span)] = both
        gate, up = both[:, :units], both[:, units:]
        at = hid.at[mine(t), pl.ds(b * units, units)]
        at[...] = (gate * jax.nn.sigmoid(gate) * up).astype(BF)
        copies.start(at, at, h_sent, share_h, at_u(1))

    @scope
    def gradients(t):
        both = summed(t, 2)
        for b in range(2):
            gate = acc[mine(t), pl.ds(b * span, units)]
            up = acc[mine(t), pl.ds(b * span + units, units)]
            grad = both[:, b * units : (b + 1) * units]
            logistic = jax.nn.sigmoid(gate)
            dgu[mine(t), pl.ds(b * span, units)] = (
                grad * up * logistic * (1.0 + gate * (1.0 - logistic))
            ).astype(BF)
            dgu[mine(t), pl.ds(b * span + units, units)] = (grad * (gate * logistic)).astype(BF)
        at = dgu.at[mine(t)]
        copies.start(at, at, d_sent, share_d + t, at_u(1))

    @scope
    def hidden_here():
        copies.arrived(hid.at[pl.ds(0, rows)], share_h, at_u(1))

    @scope
    def gradients_here(t):
        copies.arrived(dgu.at[theirs(t)], share_d + t, at_u(1))

    grad_cut = cut(quarter, GRAD_CUT)
    gr = copies.slots(3)
    gr_sent = copies.sender(gterm)

    @scope
    def flip_hidden():
        hid_t[...] = hid[...].T

    @scope
    def flip_gradients(b):
        dgu_t[pl.ds(b * span, span)] = dgu[:, pl.ds(b * span, span)].T

    @scope
    def down_out(i):
        cols = pl.ds(*grad_cut[i])
        gterm[2, :, cols] = lax.dot_general(
            hid_t[pl.ds(units, units)], xs[1, :, cols], NN, preferred_element_type=F32
        ).astype(BF)
        copies.start(gterm.at[2, :, cols], grecv.at[2, :, cols], gr_sent, gr + 2, weight_y)

    @scope
    def gate_up_out(i):
        cols = pl.ds(*grad_cut[i])
        for w in range(2):
            gterm[w, :, cols] = lax.dot_general(
                dgu_t[pl.ds(span + w * units, units)], xs[0, :, cols], NN, preferred_element_type=F32
            ).astype(BF)
            copies.start(gterm.at[w, :, cols], grecv.at[w, :, cols], gr_sent, gr + w, weight_y)

    @scope
    def term_here(w):
        left = hid_t.at[pl.ds(0, units)] if w == 2 else dgu_t.at[pl.ds(w * units, units)]
        for lo, width in grad_cut:
            cols = pl.ds(lo, width)
            gown[w, :, cols] = lax.dot_general(
                left[...], xs[w // 2, :, cols], NN, preferred_element_type=F32
            ).astype(BF)

    @scope
    def grad_out(w, ref):
        copies.arrived(grecv.at[w], gr + w, weight_y)
        ref[...] = (gown[w].astype(F32) + grecv[w].astype(F32)).astype(BF)

    parts = cut(quarter, OUT_CUT)
    dxy = copies.slots(len(parts))
    dxz, dxu = copies.slots(len(parts)), copies.slots(len(parts))
    dxy_sent = copies.sender(dx_send)
    dxz_sent = copies.sender(dxs.at[pl.ds(0, rows - rows // planes)])
    dxu_sent = copies.sender(dxs.at[pl.ds(0, rows - block)])

    def dx_term(t, cols):
        return lax.dot_general(
            dgu[pl.ds(t * rows, rows)], wgu[:, cols], NN, preferred_element_type=F32
        )

    @scope
    def dx_out(i):
        cols = pl.ds(*parts[i])
        dx_send[:, cols] = dx_term(1, cols).astype(BF)
        copies.start(dx_send.at[:, cols], dx_recv.at[:, cols], dxy_sent, dxy + i, token_y)

    @scope
    def dx_here(i):
        cols = pl.ds(*parts[i])
        dx_own[:, cols] = dx_term(0, cols)

    @scope
    def dx_z(i):
        cols = pl.ds(*parts[i])
        copies.arrived(dx_recv.at[:, cols], dxy + i, token_y)
        dxs[:, cols] = (dx_own[:, cols] + dx_recv[:, cols].astype(F32)).astype(BF)
        for k in reversed(z_order):
            copies.start(
                dxs.at[blk(z_to(k)), cols], rz.at[blk(z), cols], dxz_sent, dxz + i, at_z(k)
            )
        rz[blk(z), cols] = dxs[blk(z), cols]

    @scope
    def dx_u(i):
        cols = pl.ds(*parts[i])
        copies.arrived(rz.at[pl.ds(0, rows - rows // planes), cols], dxz + i, at_z(1))
        rzp[:, cols] = lax.dot_general(
            perm_t_ref[...], rz[:, cols], NN, preferred_element_type=F32
        ).astype(BF)
        for k in u_order:
            copies.start(
                rzp.at[blk(in_plane(k)), cols], ret.at[u, :, cols], dxu_sent, dxu + i, at_u(k)
            )
        ret[u, :, cols] = rzp[blk(u), cols]

    @scope
    def dx_back(i):
        lo, width = parts[i]
        cols = pl.ds(lo, width)
        copies.arrived(rz.at[pl.ds(0, rows - block), cols], dxu + i, at_u(1))
        for q in range(GROUP):
            total = None
            for h in range(plane // GROUP):
                got = lax.dot_general(
                    sel_t_ref[h], ret[h * GROUP + q, :, cols], NN, preferred_element_type=F32
                )
                total = got if total is None else total + got
            out_ref[:, pl.ds(q * quarter + lo, width)] = total.astype(BF)

    pltpu.make_async_copy(
        tok_hbm.at[:, pl.ds(0, GROUP * lead)], raw.at[0, :, pl.ds(0, GROUP * lead)], local_sem.at[5]
    ).wait()
    for load in loads[1:]:
        load.start()
    gather(0, 0)
    gather(0, 1)
    with jax.named_scope("barrier"):
        pl.semaphore_wait(barrier, len(partners))
    for w, (ref, _, there) in enumerate(own_w):
        copies.start(ref, there, w_sent, w_slot + w, weight_y)
    to_plane(0, 1)
    early_z()
    loads[0].wait()
    for j in range(2, 5):
        gather(0, j)
        to_plane(0, j)
    loads[1].wait()
    gather(1, 0)
    gather(1, 1)
    plane_stage(0, 1)
    early_plane()
    plane_stage(0, 2)
    to_plane(1, 0)
    to_plane(1, 1)
    gather(1, 2)
    to_plane(1, 2)
    gather(1, 3)
    to_plane(1, 3)
    forward(0, 1, 0, 4)
    plane_stage(0, 3)
    forward(0, 2, 0, 2)
    early_here(0)
    forward(0, 2, 2, 4)
    plane_stage(0, 4)
    forward(0, 3, 0, 1)
    early_here(1)
    forward(0, 3, 1, 4)
    plane_stage(1, 0)
    forward(0, 4, 0, 4)
    plane_stage(1, 1)
    weight_here(0)
    weight_here(1)
    gate_up(0, 0)
    to_core(0, 0)
    forward(1, 0, 0, 1)
    to_chip(0, 0)
    for j in range(1, 5):
        forwarded(0, j)
    gate_up(1, 0)
    to_core(1, 0)
    forward(1, 0, 1, 2)
    weight(0)
    weight(1)
    gate_up(0, 1)
    to_core(0, 1)
    to_chip(1, 0)
    gate_up(1, 1)
    to_core(1, 1)
    forward(1, 0, 2, 4)
    to_chip(0, 1)
    plane_stage(1, 2)
    to_chip(1, 1)
    plane_stage(1, 3)
    forward(1, 1, 0, 1)
    hidden(0, 0)
    forward(1, 1, 1, 4)
    hidden(1, 0)
    forward(1, 2, 0, 2)
    hidden(0, 1)
    forward(1, 2, 2, 3)
    hidden(1, 1)
    hidden_here()
    flip_hidden()
    forwarded(1, 0)
    down_out(0)
    forward(1, 2, 3, 4)
    forward(1, 3, 0, 1)
    forwarded(1, 1)
    down_out(1)
    weight_here(2)
    weight(2)
    forward(1, 3, 1, 2)
    back(0, 0, 2)
    forward(1, 3, 2, 3)
    back(1, 0, 1)
    forward(1, 3, 3, 4)
    back(0, 3, 3)
    to_core(0, 2)
    forwarded(1, 2)
    back(1, 2, 2)
    to_chip(0, 2)
    forwarded(1, 3)
    back(1, 3, 3)
    to_core(1, 2)
    down_out(2)
    to_chip(1, 2)
    gradients(0)
    down_out(3)
    gradients(1)
    gradients_here(0)
    gradients_here(1)
    dx_out(0)
    flip_gradients(1)
    gate_up_out(0)
    dx_out(1)
    gate_up_out(1)
    dx_out(2)
    dx_here(0)
    dx_out(3)
    gate_up_out(2)
    dx_z(0)
    dx_out(4)
    gate_up_out(3)
    dx_out(5)
    dx_here(1)
    dx_z(1)
    dx_out(6)
    dx_out(7)
    dx_here(2)
    dx_here(3)
    dx_z(2)
    dx_u(0)
    dx_here(4)
    dx_here(5)
    dx_z(3)
    dx_u(1)
    dx_here(6)
    dx_here(7)
    flip_gradients(0)
    dx_z(4)
    dx_u(2)
    dx_back(0)
    term_here(2)
    dx_z(5)
    dx_u(3)
    dx_back(1)
    term_here(0)
    dx_z(6)
    dx_u(4)
    dx_back(2)
    dx_z(7)
    term_here(1)
    dx_u(5)
    dx_back(3)
    dx_u(6)
    dx_back(4)
    dx_u(7)
    grad_out(2, od_ref)
    dx_back(5)
    dx_back(6)
    dx_back(7)
    grad_out(0, og_ref)
    grad_out(1, ou_ref)
    with jax.named_scope("drain"):
        copies.drain(token_y)
    assert (copies.sends, copies.recvs) == (SENDERS, receivers(planes))


def store(*refs):
    sems = refs[-1]
    moves = [pltpu.make_async_copy(refs[i], refs[4 + i], sems.at[i]) for i in range(4)]
    for move in moves:
        move.start()
    for move in moves:
        move.wait()


def body(planes, plane, capacity, tokens, out_grad, route_weight, expert_ids, w_gate, w_up, w_down):
    count, width = tokens.shape
    quarter = width // GROUP
    units = w_gate.shape[0]
    block = planes * capacity
    rows = plane * block
    half = rows // 2
    sides = plane // GROUP
    vmem = pl.BlockSpec(memory_space=pltpu.VMEM)
    hbm = pl.BlockSpec(memory_space=pl.ANY)
    results = pl.pallas_call(
        functools.partial(kernel, planes, plane, capacity),
        out_shape=(
            pltpu.VMEM((count, width), BF),
            pltpu.VMEM((units, quarter), BF),
            pltpu.VMEM((units, quarter), BF),
            pltpu.VMEM((units, quarter), BF),
        ),
        in_specs=[vmem] * 2 + [hbm] * 5,
        out_specs=(vmem,) * 4,
        scratch_shapes=[
            pltpu.VMEM((sides * block, count), BF),
            pltpu.VMEM((sides, count, block), BF),
            pltpu.VMEM((sides * block, 1), F32),
            pltpu.VMEM((rows, rows), BF),
            pltpu.VMEM((rows, rows), BF),
            pltpu.VMEM((2, count, width), BF),
            pltpu.VMEM((2, rows, quarter), BF),
            pltpu.VMEM((rows, quarter // 14 * IN_CUTS[0][0]), BF),
            pltpu.VMEM((rows, quarter // 14 * IN_CUTS[0][0]), BF),
            pltpu.VMEM((rows, quarter // 14 * IN_CUTS[0][0]), BF),
            pltpu.VMEM((2, rows, quarter), BF),
            pltpu.VMEM((2, rows, quarter), BF),
            pltpu.VMEM((2, 2 * rows, quarter), BF),
            pltpu.VMEM((4 * units, quarter), BF),
            pltpu.VMEM((2 * units, quarter), BF),
            pltpu.VMEM((2 * rows, 6 * units), F32),
            pltpu.VMEM((2, half, 6 * units), BF),
            pltpu.VMEM((2, half, 6 * units), BF),
            pltpu.VMEM((2, half, 6 * units), BF),
            pltpu.VMEM((2, half, 6 * units), BF),
            pltpu.VMEM((2 * rows, 2 * units), BF),
            pltpu.VMEM((2 * units, 2 * rows), BF),
            pltpu.VMEM((2 * rows, 4 * units), BF),
            pltpu.VMEM((4 * units, 2 * rows), BF),
            pltpu.VMEM((3, units, quarter), BF),
            pltpu.VMEM((3, units, quarter), BF),
            pltpu.VMEM((3, units, quarter), BF),
            pltpu.VMEM((rows, quarter), BF),
            pltpu.VMEM((rows, quarter), BF),
            pltpu.VMEM((rows, quarter), F32),
            pltpu.VMEM((rows, quarter), BF),
            pltpu.VMEM((rows, quarter), BF),
            pltpu.VMEM((rows, quarter), BF),
            pltpu.VMEM((plane, block, quarter), BF),
            pltpu.SemaphoreType.DMA((6,)),
            pltpu.SemaphoreType.DMA((SENDERS,)),
            pltpu.SemaphoreType.DMA((receivers(planes),)),
        ],
        compiler_params=pltpu.CompilerParams(
            collective_id=0, has_side_effects=True, vmem_limit_bytes=58 * 1024 * 1024
        ),
        name="expert_backward",
    )(
        expert_ids.reshape(1, count), route_weight.reshape(1, count),
        tokens, out_grad, w_gate, w_up, w_down,
    )
    return pl.pallas_call(
        store,
        out_shape=tuple(jax.ShapeDtypeStruct(a.shape, a.dtype) for a in results),
        in_specs=[vmem] * 4,
        out_specs=(hbm,) * 4,
        scratch_shapes=[pltpu.SemaphoreType.DMA((4,))],
        compiler_params=pltpu.CompilerParams(vmem_limit_bytes=1024 * 1024),
        name="store",
    )(*(pltpu.with_memory_space_constraint(a, pltpu.VMEM) for a in results))


def solution(mesh):
    tokens = P(("dp", "ep"), None)
    weights = P("dp", "ep")
    planes = mesh.shape["ep"] // PLANE
    return jax.shard_map(
        functools.partial(body, planes, PLANE, CAP),
        mesh=mesh,
        in_specs=(tokens, tokens, tokens, tokens, weights, weights, weights),
        out_specs=(tokens, weights, weights, weights),
        check_vma=False,
    )
```

```python
import functools

import jax
import jax.numpy as jnp
from jax import lax
from jax.experimental import pallas as pl
from jax.experimental.pallas import tpu as pltpu
from jax.sharding import PartitionSpec as P

D = 7168
GROUP = 4
CAP = 6
PLANE = 8
NT = (((1,), (1,)), ((), ()))
NN = (((1,), (0,)), ((), ()))
MESH = pl.DeviceIdType.MESH
BF = jnp.bfloat16
F32 = jnp.float32


def scope(stage):
    @functools.wraps(stage)
    def named(*args):
        tag = "_".join(str(a) for a in args if isinstance(a, int))
        with jax.named_scope(f"{stage.__name__}_{tag}"):
            return stage(*args)

    return named


class Copies:
    def __init__(self, send, recv):
        self.send, self.recv, self.sends, self.recvs, self.open = send, recv, 0, 0, []

    def sender(self, whole):
        self.open.append((whole, self.sends))
        self.sends += 1
        return self.sends - 1

    def slots(self, count):
        self.recvs += count
        return self.recvs - count

    def make(self, src, dst, sent, slot, device):
        return pltpu.make_async_remote_copy(
            src_ref=src,
            dst_ref=dst,
            send_sem=self.send.at[sent],
            recv_sem=self.recv.at[slot],
            device_id=device,
            device_id_type=MESH,
        )

    def start(self, src, dst, sent, slot, device):
        self.make(src, dst, sent, slot, device).start()

    def arrived(self, whole, slot, device):
        self.make(whole, whole, 0, slot, device).wait_recv()

    def drain(self, device):
        for whole, sent in self.open:
            self.make(whole, whole, sent, 0, device).wait_send()


def cut(width, sizes):
    unit, at, out = width // 14, 0, []
    for size in sizes:
        out.append((at, size * unit))
        at += size * unit
    return out


IN_CUTS = ((2, 2, 3, 4, 3), (4, 4, 4, 2))
OUT_CUT = (2, 2, 2, 2, 2, 2, 1, 1)
GRAD_CUT = (4, 4, 4, 2)
SENDERS = 15


def receivers(planes):
    chunks = len(IN_CUTS[0]) + len(IN_CUTS[1])
    return chunks * (2 + planes // 2) - planes // 2 + 1 + 3 * len(OUT_CUT) + 3 + 6 + 6 + 1 + 2 + 3


def slot_tables(planes, plane, cap, ids_ref, rw_ref, sel_ref, sel_t_ref, scale_ref, perm_ref, perm_t_ref):
    count = ids_ref.shape[1]
    block, rows, sides = planes * cap, perm_ref.shape[0], plane // GROUP
    by_col = jnp.broadcast_to(ids_ref[...].astype(F32), (count, count))
    by_row = by_col.T
    i = lax.broadcasted_iota(jnp.int32, (count, count), 0)
    j = lax.broadcasted_iota(jnp.int32, (count, count), 1)
    same = by_col == by_row
    rank_col = jnp.sum(jnp.where(same & (i < j), 1.0, 0.0), axis=0, keepdims=True)
    rank_row = jnp.sum(jnp.where(same & (j < i), 1.0, 0.0), axis=1, keepdims=True)

    def wanted(shape, axis, side_rows):
        at = lax.broadcasted_iota(jnp.int32, shape, axis)
        side, at = at // side_rows, lax.rem(at, side_rows)
        expert = at // cap * sides + side
        return expert.astype(F32), lax.rem(at, cap).astype(F32)

    expert, rank = wanted((sides * block, count), 0, block)
    match = (by_col[:1] == expert) & (rank_col == rank)
    sel_ref[...] = jnp.where(match, 1.0, 0.0).astype(BF)
    scale_ref[...] = jnp.sum(jnp.where(match, rw_ref[...], 0.0), axis=1, keepdims=True)
    expert, rank = wanted((count, block), 1, block)
    for side in range(sides):
        match = (by_row[:, :1] == expert + float(side)) & (rank_row == rank)
        sel_t_ref[side] = jnp.where(match, 1.0, 0.0).astype(BF)

    def source(shape, axis):
        at = lax.broadcasted_iota(jnp.int32, shape, axis)
        zi, rest = at // (plane * cap), lax.rem(at, plane * cap)
        return rest // cap * block + zi * cap + lax.rem(rest, cap)

    i = lax.broadcasted_iota(jnp.int32, (rows, rows), 0)
    j = lax.broadcasted_iota(jnp.int32, (rows, rows), 1)
    perm_ref[...] = jnp.where(source((rows, 1), 0) == j, 1.0, 0.0).astype(BF)
    perm_t_ref[...] = jnp.where(source((1, rows), 1) == i, 1.0, 0.0).astype(BF)


def kernel(
    planes, plane, cap,
    ids_ref, rw_ref, tok_hbm, grad_hbm, wg_hbm, wu_hbm, wd_hbm,
    out_ref, og_ref, ou_ref, od_ref,
    sel_ref, sel_t_ref, scale_ref, perm_ref, perm_t_ref, raw,
    send1, ez, ez_in, er, r1, r1p, xs, wgu, wdn, acc, core_out, core_in, chip_out, chip_in,
    hid, hid_t, dgu, dgu_t, gterm, gown, grecv, dx_send, dx_recv, dx_own, dxs, rz, rzp, ret,
    local_sem, send_sem, recv_sem,
):
    quarter = xs.shape[2]
    block = planes * cap
    rows = plane * block
    half = rows // 2
    units = hid.shape[1] // 2
    r = lax.axis_index("dp")
    ep = lax.axis_index("ep")
    z = ep // plane
    u = lax.rem(ep, plane)
    c = lax.rem(u, 2)
    copies = Copies(send_sem, recv_sem)

    def in_plane(k):
        out = u
        for bit in range(3):
            if k >> bit & 1:
                out = out + (1 << bit) * (1 - 2 * lax.rem(u // (1 << bit), 2))
        return out

    def at_u(k):
        return (r, z * plane + in_plane(k))

    def across(k):
        return (r + 1 - 2 * lax.rem(r, 2), z * plane + in_plane(k))

    def z_to(k):
        return lax.rem(z + k, planes)

    def z_from(k):
        return lax.rem(z + planes - k, planes)

    def at_z(k):
        return (r, z_to(k) * plane + u)

    def from_z(k):
        return (r, z_from(k) * plane + u)

    def blk(index):
        return pl.ds(pl.multiple_of(index * block, block), block)

    def other(index):
        return pl.ds(pl.multiple_of(rows + index * block, block), block)

    reach = [sorted({k, planes - k}) for k in range(1, planes // 2 + 1)]
    z_order = [k for group in reach for k in group]
    u_order = [k for k in (4, 5, 2, 3, 6, 7, 1) if k < plane]
    token_y, weight_y = (r + 1 - 2 * lax.rem(r, 2), ep), (3 - r, ep)

    own_w = (
        (wg_hbm, wgu.at[pl.ds(0, units)], wgu.at[pl.ds(2 * units, units)]),
        (wu_hbm, wgu.at[pl.ds(units, units)], wgu.at[pl.ds(3 * units, units)]),
        (wd_hbm, wdn.at[pl.ds(0, units)], wdn.at[pl.ds(units, units)]),
    )
    lead = quarter // 14 * sum(IN_CUTS[0][:2])
    ahead = [
        pltpu.make_async_copy(
            tok_hbm.at[:, pl.ds(q * quarter + lo, width)],
            raw.at[0, :, pl.ds(q * quarter + lo, width)],
            local_sem.at[n],
        )
        for n, lo, width in ((5, 0, lead), (0, lead, quarter - lead))
        for q in range(GROUP)
    ]
    loads = [
        pltpu.make_async_copy(tok_hbm.at[:, pl.ds(0, GROUP * (quarter - lead))], raw.at[0, :, pl.ds(0, GROUP * (quarter - lead))], local_sem.at[0]),
        pltpu.make_async_copy(grad_hbm, raw.at[1], local_sem.at[1]),
    ]
    for w, (ref, here, _) in enumerate(own_w):
        loads.append(pltpu.make_async_copy(ref, here, local_sem.at[2 + w]))
    for load in ahead:
        load.start()

    barrier = pltpu.get_barrier_semaphore()
    partners = [at_u(k) for k in u_order] + [at_z(k) for k in z_order] + [token_y, weight_y]
    partners += [across(k) for k in u_order]
    for device in partners:
        pl.semaphore_signal(barrier, inc=1, device_id=device, device_id_type=MESH)

    with jax.named_scope("tables"):
        slot_tables(
            planes, plane, cap, ids_ref, rw_ref, sel_ref, sel_t_ref, scale_ref, perm_ref, perm_t_ref
        )
    w_slot = copies.slots(3)
    w_sent = copies.sender(wgu.at[pl.ds(0, 3 * units)])

    @scope
    def weight_here(w):
        loads[2 + w].wait()

    @scope
    def weight(w):
        copies.arrived(own_w[w][2], w_slot + w, weight_y)

    chunks = [cut(quarter, sizes) for sizes in IN_CUTS]
    index = [[0, 1, 2, 3, 4], [5, 6, 7, 8]]
    total = len(IN_CUTS[0]) + len(IN_CUTS[1])
    st1, fwd = copies.slots(total), copies.slots(total)
    early, st2 = copies.slots(1), copies.slots((total - 1) * len(reach)) - len(reach)
    st1_sent = [copies.sender(r1p.at[a, pl.ds(0, rows - block)]) for a in range(2)]
    st2_sent = [copies.sender(r1p.at[a, pl.ds(0, rows - rows // planes)]) for a in range(2)]
    fwd_sent = [copies.sender(xs.at[a, pl.ds(0, rows)]) for a in range(2)]

    @scope
    def gather(a, j):
        lo, width = chunks[a][j]
        cols = pl.ds(lo, width)
        for q in range(GROUP):
            got = lax.dot_general(
                sel_ref[...], raw[a, :, pl.ds(q * quarter + lo, width)], NN, preferred_element_type=F32
            )
            if a:
                got = got * scale_ref[...]
            got = got.astype(BF)
            for h in range(plane // GROUP):
                send1[a, pl.ds((h * GROUP + q) * block, block), cols] = got[h * block : (h + 1) * block]

    @scope
    def to_plane(a, j):
        cols = pl.ds(*chunks[a][j])
        r1[a, blk(u), cols] = send1[a, blk(u), cols]
        for k in u_order:
            copies.start(
                send1.at[a, blk(in_plane(k)), cols],
                r1.at[a, blk(u), cols],
                st1_sent[a],
                st1 + index[a][j],
                at_u(k),
            )

    @scope
    def plane_stage(a, j):
        cols = pl.ds(*chunks[a][j])
        copies.arrived(r1.at[a, pl.ds(0, rows - block), cols], st1 + index[a][j], at_u(1))
        r1p[a, :, cols] = lax.dot_general(
            perm_ref[...], r1[a, :, cols], NN, preferred_element_type=F32
        ).astype(BF)
        for g, group in enumerate(reach):
            for k in group:
                copies.start(
                    r1p.at[a, blk(z_to(k)), cols],
                    xs.at[a, blk(z), cols],
                    st2_sent[a],
                    st2 + index[a][j] * len(reach) + g,
                    at_z(k),
                )
        xs[a, blk(z), cols] = r1p[a, blk(z), cols]
        pass_on(a, j, 0)

    first = pl.ds(*chunks[0][0])

    @scope
    def early_z():
        ez[...] = lax.dot_general(
            perm_ref[...], send1[0, :, first], NN, preferred_element_type=F32
        ).astype(BF)
        for k in z_order:
            copies.start(ez.at[blk(z_to(k))], ez_in.at[blk(z)], st2_sent[0], early, at_z(k))
        ez_in[blk(z)] = ez[blk(z)]

    @scope
    def early_plane():
        copies.arrived(ez_in.at[pl.ds(0, rows - rows // planes)], early, at_z(1))
        r1p[0, :, first] = lax.dot_general(
            perm_t_ref[...], ez_in[...], NN, preferred_element_type=F32
        ).astype(BF)
        for k in u_order:
            copies.start(
                r1p.at[0, blk(in_plane(k)), first], r1.at[0, blk(u), first], st1_sent[0], st1, at_u(k)
            )
        for k in [0] + u_order:
            copies.start(
                r1p.at[0, blk(in_plane(k)), first], er.at[blk(u)], fwd_sent[0], fwd, across(k)
            )
        r1[0, blk(u), first] = r1p[0, blk(u), first]

    @scope
    def early_here(t):
        if t:
            copies.arrived(er, fwd, token_y)
        else:
            copies.arrived(r1.at[0, pl.ds(0, rows - block), first], st1, at_u(1))
        src = er[...] if t else r1[0, :, first]
        xs[0, pl.ds(t * rows, rows), first] = lax.dot_general(
            perm_ref[...], src, NN, preferred_element_type=F32
        ).astype(BF)

    @scope
    def forward(a, j, g0, g1):
        cols = pl.ds(*chunks[a][j])
        for g in range(g0, min(g1, len(reach))):
            copies.arrived(
                xs.at[a, pl.ds(0, len(reach[g]) * block), cols],
                st2 + index[a][j] * len(reach) + g,
                at_z(1),
            )
            for k in reach[g]:
                pass_on(a, j, k)

    def pass_on(a, j, k):
        cols = pl.ds(*chunks[a][j])
        zs = z_from(k)
        copies.start(
            xs.at[a, blk(zs), cols], xs.at[a, other(zs), cols], fwd_sent[a], fwd + index[a][j], token_y
        )

    @scope
    def forwarded(a, j):
        cols = pl.ds(*chunks[a][j])
        copies.arrived(xs.at[a, pl.ds(rows, rows), cols], fwd + index[a][j], token_y)

    mine = lambda t: pl.ds(pl.multiple_of(t * rows + c * half, half), half)
    theirs = lambda t: pl.ds(pl.multiple_of(t * rows + (1 - c) * half, half), half)
    core = copies.slots(6)
    chip = copies.slots(6)
    share_h, share_d = copies.slots(1), copies.slots(2)
    core_sent, chip_sent = copies.sender(core_out), copies.sender(chip_out)
    h_sent, d_sent = copies.sender(hid.at[pl.ds(0, rows)]), copies.sender(dgu.at[pl.ds(0, rows)])
    span = 2 * units

    def project(left, weights, t, g, cols, add):
        at = pl.ds(t * rows, rows)

        def step(b, carry):
            got = lax.dot_general(
                left[at, cols],
                weights[pl.ds(pl.multiple_of(b * units, units), units), cols],
                NT,
                preferred_element_type=F32,
            )
            to = pl.ds(pl.multiple_of(g * span + b * units, units), units)
            acc[at, to] = acc[at, to] + got if add else got
            return carry

        lax.fori_loop(0, 2, step, 0)

    @scope
    def gate_up(t, b):
        project(xs.at[0], wgu.at[pl.ds(b * span, span)], t, b, pl.ds(0, quarter), False)

    @scope
    def back(t, j0, j1):
        lo = chunks[1][j0][0]
        width = sum(chunks[1][j1]) - lo
        project(xs.at[1], wdn, t, 2, pl.ds(lo, width), j0 > 0)

    @scope
    def to_core(t, g):
        cols = pl.ds(g * span, span)
        core_out[t, :, cols] = acc[theirs(t), cols].astype(BF)
        copies.start(core_out.at[t, :, cols], core_in.at[t, :, cols], core_sent, core + 3 * t + g, at_u(1))

    @scope
    def to_chip(t, g):
        cols = pl.ds(g * span, span)
        copies.arrived(core_in.at[t, :, cols], core + 3 * t + g, at_u(1))
        pair = acc[mine(t), cols] + core_in[t, :, cols].astype(F32)
        acc[mine(t), cols] = pair
        chip_out[t, :, cols] = pair.astype(BF)
        copies.start(chip_out.at[t, :, cols], chip_in.at[t, :, cols], chip_sent, chip + 3 * t + g, at_u(2))

    def summed(t, g):
        cols = pl.ds(g * span, span)
        copies.arrived(chip_in.at[t, :, cols], chip + 3 * t + g, at_u(2))
        return acc[mine(t), cols] + chip_in[t, :, cols].astype(F32)

    @scope
    def hidden(t, b):
        both = summed(t, b)
        acc[mine(t), pl.ds(b * span, span)] = both
        gate, up = both[:, :units], both[:, units:]
        at = hid.at[mine(t), pl.ds(b * units, units)]
        at[...] = (gate * jax.nn.sigmoid(gate) * up).astype(BF)
        copies.start(at, at, h_sent, share_h, at_u(1))

    @scope
    def gradients(t):
        both = summed(t, 2)
        for b in range(2):
            gate = acc[mine(t), pl.ds(b * span, units)]
            up = acc[mine(t), pl.ds(b * span + units, units)]
            grad = both[:, b * units : (b + 1) * units]
            logistic = jax.nn.sigmoid(gate)
            dgu[mine(t), pl.ds(b * span, units)] = (
                grad * up * logistic * (1.0 + gate * (1.0 - logistic))
            ).astype(BF)
            dgu[mine(t), pl.ds(b * span + units, units)] = (grad * (gate * logistic)).astype(BF)
        at = dgu.at[mine(t)]
        copies.start(at, at, d_sent, share_d + t, at_u(1))

    @scope
    def hidden_here():
        copies.arrived(hid.at[pl.ds(0, rows)], share_h, at_u(1))

    @scope
    def gradients_here(t):
        copies.arrived(dgu.at[theirs(t)], share_d + t, at_u(1))

    grad_cut = cut(quarter, GRAD_CUT)
    gr = copies.slots(3)
    gr_sent = copies.sender(gterm)

    @scope
    def flip_hidden():
        hid_t[...] = hid[...].T

    @scope
    def flip_gradients(b):
        dgu_t[pl.ds(b * span, span)] = dgu[:, pl.ds(b * span, span)].T

    @scope
    def down_out(i):
        cols = pl.ds(*grad_cut[i])
        gterm[2, :, cols] = lax.dot_general(
            hid_t[pl.ds(units, units)], xs[1, :, cols], NN, preferred_element_type=F32
        ).astype(BF)
        copies.start(gterm.at[2, :, cols], grecv.at[2, :, cols], gr_sent, gr + 2, weight_y)

    @scope
    def gate_up_out(i):
        cols = pl.ds(*grad_cut[i])
        for w in range(2):
            gterm[w, :, cols] = lax.dot_general(
                dgu_t[pl.ds(span + w * units, units)], xs[0, :, cols], NN, preferred_element_type=F32
            ).astype(BF)
            copies.start(gterm.at[w, :, cols], grecv.at[w, :, cols], gr_sent, gr + w, weight_y)

    @scope
    def term_here(w):
        left = hid_t.at[pl.ds(0, units)] if w == 2 else dgu_t.at[pl.ds(w * units, units)]
        for lo, width in grad_cut:
            cols = pl.ds(lo, width)
            gown[w, :, cols] = lax.dot_general(
                left[...], xs[w // 2, :, cols], NN, preferred_element_type=F32
            ).astype(BF)

    @scope
    def grad_out(w, ref):
        copies.arrived(grecv.at[w], gr + w, weight_y)
        ref[...] = (gown[w].astype(F32) + grecv[w].astype(F32)).astype(BF)

    parts = cut(quarter, OUT_CUT)
    dxy = copies.slots(len(parts))
    dxz, dxu = copies.slots(len(parts)), copies.slots(len(parts))
    dxy_sent = copies.sender(dx_send)
    dxz_sent = copies.sender(dxs.at[pl.ds(0, rows - rows // planes)])
    dxu_sent = copies.sender(dxs.at[pl.ds(0, rows - block)])

    def dx_term(t, cols):
        return lax.dot_general(
            dgu[pl.ds(t * rows, rows)], wgu[:, cols], NN, preferred_element_type=F32
        )

    @scope
    def dx_out(i):
        cols = pl.ds(*parts[i])
        dx_send[:, cols] = dx_term(1, cols).astype(BF)
        copies.start(dx_send.at[:, cols], dx_recv.at[:, cols], dxy_sent, dxy + i, token_y)

    @scope
    def dx_here(i):
        cols = pl.ds(*parts[i])
        dx_own[:, cols] = dx_term(0, cols)

    @scope
    def dx_z(i):
        cols = pl.ds(*parts[i])
        copies.arrived(dx_recv.at[:, cols], dxy + i, token_y)
        dxs[:, cols] = (dx_own[:, cols] + dx_recv[:, cols].astype(F32)).astype(BF)
        for k in reversed(z_order):
            copies.start(
                dxs.at[blk(z_to(k)), cols], rz.at[blk(z), cols], dxz_sent, dxz + i, at_z(k)
            )
        rz[blk(z), cols] = dxs[blk(z), cols]

    @scope
    def dx_u(i):
        cols = pl.ds(*parts[i])
        copies.arrived(rz.at[pl.ds(0, rows - rows // planes), cols], dxz + i, at_z(1))
        rzp[:, cols] = lax.dot_general(
            perm_t_ref[...], rz[:, cols], NN, preferred_element_type=F32
        ).astype(BF)
        for k in u_order:
            copies.start(
                rzp.at[blk(in_plane(k)), cols], ret.at[u, :, cols], dxu_sent, dxu + i, at_u(k)
            )
        ret[u, :, cols] = rzp[blk(u), cols]

    @scope
    def dx_back(i):
        lo, width = parts[i]
        cols = pl.ds(lo, width)
        copies.arrived(rz.at[pl.ds(0, rows - block), cols], dxu + i, at_u(1))
        for q in range(GROUP):
            total = None
            for h in range(plane // GROUP):
                got = lax.dot_general(
                    sel_t_ref[h], ret[h * GROUP + q, :, cols], NN, preferred_element_type=F32
                )
                total = got if total is None else total + got
            out_ref[:, pl.ds(q * quarter + lo, width)] = total.astype(BF)

    pltpu.make_async_copy(
        tok_hbm.at[:, pl.ds(0, GROUP * lead)], raw.at[0, :, pl.ds(0, GROUP * lead)], local_sem.at[5]
    ).wait()
    for load in loads[1:]:
        load.start()
    gather(0, 0)
    gather(0, 1)
    with jax.named_scope("barrier"):
        pl.semaphore_wait(barrier, len(partners))
    for w, (ref, _, there) in enumerate(own_w):
        copies.start(ref, there, w_sent, w_slot + w, weight_y)
    to_plane(0, 1)
    early_z()
    loads[0].wait()
    for j in range(2, 5):
        gather(0, j)
        to_plane(0, j)
    loads[1].wait()
    gather(1, 0)
    gather(1, 1)
    plane_stage(0, 1)
    early_plane()
    plane_stage(0, 2)
    to_plane(1, 0)
    to_plane(1, 1)
    gather(1, 2)
    to_plane(1, 2)
    gather(1, 3)
    to_plane(1, 3)
    forward(0, 1, 0, 4)
    plane_stage(0, 3)
    forward(0, 2, 0, 2)
    early_here(0)
    forward(0, 2, 2, 4)
    plane_stage(0, 4)
    forward(0, 3, 0, 1)
    early_here(1)
    forward(0, 3, 1, 4)
    plane_stage(1, 0)
    forward(0, 4, 0, 4)
    plane_stage(1, 1)
    weight_here(0)
    weight_here(1)
    gate_up(0, 0)
    to_core(0, 0)
    forward(1, 0, 0, 1)
    to_chip(0, 0)
    for j in range(1, 5):
        forwarded(0, j)
    gate_up(1, 0)
    to_core(1, 0)
    forward(1, 0, 1, 2)
    weight(0)
    weight(1)
    gate_up(0, 1)
    to_core(0, 1)
    to_chip(1, 0)
    gate_up(1, 1)
    to_core(1, 1)
    forward(1, 0, 2, 4)
    to_chip(0, 1)
    plane_stage(1, 2)
    to_chip(1, 1)
    plane_stage(1, 3)
    forward(1, 1, 0, 1)
    hidden(0, 0)
    forward(1, 1, 1, 4)
    hidden(1, 0)
    forward(1, 2, 0, 2)
    hidden(0, 1)
    forward(1, 2, 2, 3)
    hidden(1, 1)
    hidden_here()
    flip_hidden()
    forwarded(1, 0)
    down_out(0)
    forward(1, 2, 3, 4)
    forward(1, 3, 0, 1)
    forwarded(1, 1)
    down_out(1)
    weight_here(2)
    weight(2)
    forward(1, 3, 1, 2)
    back(0, 0, 2)
    forward(1, 3, 2, 3)
    back(1, 0, 1)
    forward(1, 3, 3, 4)
    back(0, 3, 3)
    to_core(0, 2)
    forwarded(1, 2)
    back(1, 2, 2)
    to_chip(0, 2)
    forwarded(1, 3)
    back(1, 3, 3)
    to_core(1, 2)
    down_out(2)
    to_chip(1, 2)
    gradients(0)
    down_out(3)
    gradients(1)
    gradients_here(0)
    gradients_here(1)
    dx_out(0)
    flip_gradients(1)
    gate_up_out(0)
    dx_out(1)
    gate_up_out(1)
    dx_out(2)
    dx_here(0)
    dx_out(3)
    gate_up_out(2)
    dx_z(0)
    dx_out(4)
    gate_up_out(3)
    dx_out(5)
    dx_here(1)
    dx_z(1)
    dx_out(6)
    dx_out(7)
    dx_here(2)
    dx_here(3)
    dx_z(2)
    dx_u(0)
    dx_here(4)
    dx_here(5)
    dx_z(3)
    dx_u(1)
    dx_here(6)
    dx_here(7)
    flip_gradients(0)
    term_here(0)
    dx_z(4)
    dx_u(2)
    dx_back(0)
    term_here(2)
    term_here(1)
    dx_z(5)
    dx_u(3)
    dx_back(1)
    dx_z(6)
    dx_u(4)
    dx_back(2)
    dx_z(7)
    dx_u(5)
    dx_back(3)
    dx_u(6)
    dx_back(4)
    dx_u(7)
    grad_out(2, od_ref)
    dx_back(5)
    dx_back(6)
    dx_back(7)
    grad_out(0, og_ref)
    grad_out(1, ou_ref)
    with jax.named_scope("drain"):
        copies.drain(token_y)
    assert (copies.sends, copies.recvs) == (SENDERS, receivers(planes))


def store(*refs):
    sems = refs[-1]
    moves = [pltpu.make_async_copy(refs[i], refs[4 + i], sems.at[i]) for i in range(4)]
    for move in moves:
        move.start()
    for move in moves:
        move.wait()


def body(planes, plane, capacity, tokens, out_grad, route_weight, expert_ids, w_gate, w_up, w_down):
    count, width = tokens.shape
    quarter = width // GROUP
    units = w_gate.shape[0]
    block = planes * capacity
    rows = plane * block
    half = rows // 2
    sides = plane // GROUP
    vmem = pl.BlockSpec(memory_space=pltpu.VMEM)
    hbm = pl.BlockSpec(memory_space=pl.ANY)
    results = pl.pallas_call(
        functools.partial(kernel, planes, plane, capacity),
        out_shape=(
            pltpu.VMEM((count, width), BF),
            pltpu.VMEM((units, quarter), BF),
            pltpu.VMEM((units, quarter), BF),
            pltpu.VMEM((units, quarter), BF),
        ),
        in_specs=[vmem] * 2 + [hbm] * 5,
        out_specs=(vmem,) * 4,
        scratch_shapes=[
            pltpu.VMEM((sides * block, count), BF),
            pltpu.VMEM((sides, count, block), BF),
            pltpu.VMEM((sides * block, 1), F32),
            pltpu.VMEM((rows, rows), BF),
            pltpu.VMEM((rows, rows), BF),
            pltpu.VMEM((2, count, width), BF),
            pltpu.VMEM((2, rows, quarter), BF),
            pltpu.VMEM((rows, quarter // 14 * IN_CUTS[0][0]), BF),
            pltpu.VMEM((rows, quarter // 14 * IN_CUTS[0][0]), BF),
            pltpu.VMEM((rows, quarter // 14 * IN_CUTS[0][0]), BF),
            pltpu.VMEM((2, rows, quarter), BF),
            pltpu.VMEM((2, rows, quarter), BF),
            pltpu.VMEM((2, 2 * rows, quarter), BF),
            pltpu.VMEM((4 * units, quarter), BF),
            pltpu.VMEM((2 * units, quarter), BF),
            pltpu.VMEM((2 * rows, 6 * units), F32),
            pltpu.VMEM((2, half, 6 * units), BF),
            pltpu.VMEM((2, half, 6 * units), BF),
            pltpu.VMEM((2, half, 6 * units), BF),
            pltpu.VMEM((2, half, 6 * units), BF),
            pltpu.VMEM((2 * rows, 2 * units), BF),
            pltpu.VMEM((2 * units, 2 * rows), BF),
            pltpu.VMEM((2 * rows, 4 * units), BF),
            pltpu.VMEM((4 * units, 2 * rows), BF),
            pltpu.VMEM((3, units, quarter), BF),
            pltpu.VMEM((3, units, quarter), BF),
            pltpu.VMEM((3, units, quarter), BF),
            pltpu.VMEM((rows, quarter), BF),
            pltpu.VMEM((rows, quarter), BF),
            pltpu.VMEM((rows, quarter), F32),
            pltpu.VMEM((rows, quarter), BF),
            pltpu.VMEM((rows, quarter), BF),
            pltpu.VMEM((rows, quarter), BF),
            pltpu.VMEM((plane, block, quarter), BF),
            pltpu.SemaphoreType.DMA((6,)),
            pltpu.SemaphoreType.DMA((SENDERS,)),
            pltpu.SemaphoreType.DMA((receivers(planes),)),
        ],
        compiler_params=pltpu.CompilerParams(
            collective_id=0, has_side_effects=True, vmem_limit_bytes=58 * 1024 * 1024
        ),
        name="expert_backward",
    )(
        expert_ids.reshape(1, count), route_weight.reshape(1, count),
        tokens, out_grad, w_gate, w_up, w_down,
    )
    return pl.pallas_call(
        store,
        out_shape=tuple(jax.ShapeDtypeStruct(a.shape, a.dtype) for a in results),
        in_specs=[vmem] * 4,
        out_specs=(hbm,) * 4,
        scratch_shapes=[pltpu.SemaphoreType.DMA((4,))],
        compiler_params=pltpu.CompilerParams(vmem_limit_bytes=1024 * 1024),
        name="store",
    )(*(pltpu.with_memory_space_constraint(a, pltpu.VMEM) for a in results))


def solution(mesh):
    tokens = P(("dp", "ep"), None)
    weights = P("dp", "ep")
    planes = mesh.shape["ep"] // PLANE
    return jax.shard_map(
        functools.partial(body, planes, PLANE, CAP),
        mesh=mesh,
        in_specs=(tokens, tokens, tokens, tokens, weights, weights, weights),
        out_specs=(tokens, weights, weights, weights),
        check_vma=False,
    )
```
